32 devices in a mesh: row: 8 (over y, x, core), col: 4 (over z).
Axes of the slice: x: 2, y: 2, z: 4, core: 2. Of those that a mesh axis runs over, the one named last changes fastest.
Arguments:
- object_field: float32 [2, 4096, 2048], P(None, 'row', 'col'), may hold values from -6 to 6
- probe: float32 [3, 2, 256, 256], replicated, may hold values from -6 to 6
- raw_counts: bfloat16 [192, 256, 256], P(('row', 'col')), may hold values from 0.099609375 to 10
- resample_delta: float32 [256, 256], replicated, may hold values from -0.1875 to 0.1875
- tile_row: int32 [192, 1], P(('row', 'col')), may hold values from 0 to 7; in each aligned block of 6 rows (0 to 5, 6 to 11, ...) no two rows name the same one
- offsets: int32 [192, 2], P(('row', 'col')), may hold values from 0 to 511
Outputs:
- object_grad: float32 [2, 4096, 2048], P(None, 'row', 'col')
- probe_grad: float32 [3, 2, 256, 256], replicated
The draws below stay inside these ranges and needn't reach their ends.
Inputs may be any that keep to these rules, and one draw needn't show every extreme that they name: `tile_row`: the 6 frames of one device have distinct tile rows.
All inputs are finite; a program needn't handle non-finite values.
Results may differ from the reference program's by a relative error of at most 0.0008.
The reference program's roundings to bfloat16 on the way count: a program that leaves them out, or rounds other values in their place, can miss the bound.
Values may be sent and summed in bfloat16 or wider, within the bound.
A program may use at most 128 MiB of HBM per device.

```python
import math
import jax
import jax.numpy as jnp
import numpy as np
from jax import lax

FRAME = 256
MODES = 3
TILE = 512
FR_DEV = 6
FRAMES = 192
OBJ_ROWS = 4096
OBJ_COLS = 2048
N_ROW = 8
N_COL = 4


def set_ends(entries, rng, low, high):
    place = [jax.random.randint(jax.random.fold_in(rng, axis), (), 0, length) for axis, length in enumerate(entries.shape)]
    longest = entries.shape.index(max(entries.shape))
    next_to = place[:longest] + [(place[longest] + 1) % entries.shape[longest]] + place[longest + 1:]
    return entries.at[tuple(place)].set(low).at[tuple(next_to)].set(high)


def level_of(stream_key, shape, pieces, least, largest):
    def one(axis_at, parts):
        steps = jax.random.uniform(jax.random.fold_in(jax.random.fold_in(stream_key, 6), axis_at), (parts,), jnp.float32, least / len(pieces), largest / len(pieces))
        return jnp.repeat(jnp.exp(steps), shape[axis_at] // parts).reshape((-1,) + (1,) * (len(shape) - axis_at - 1))

    loudness = one(*pieces[0])
    for cut in pieces[1:]:
        loudness = loudness * one(*cut)
    return loudness


def shared_out(key, own, number, rows, count, top, reach, skew):
    sequence = jax.random.permutation(key, count)
    packed, ordinary = shares(count, rows * top, reach, skew, True), shares(count, rows * top, reach, skew, False)
    places = jnp.arange(count)

    def named(lengths, turn):
        used = int((lengths > 0).sum())
        fixed = max(1, used // 4)
        shifted = fixed + (places - fixed + turn * (used - fixed)) % max(1, count - fixed)
        return jnp.zeros((count,), jnp.int32).at[sequence[jnp.where(places < fixed, places, shifted)]].set(jnp.asarray(lengths, jnp.int32))

    lengths = jnp.where(number % 4 == 0, named(packed, number // 4), named(ordinary, number - number // 4 - 1))
    mixed = jax.random.permutation(jax.random.fold_in(own, 3), count)
    giver, sink = mixed[0:count // 2 * 2:2], mixed[1:count // 2 * 2:2]
    margin = jnp.minimum(lengths[giver] - 1, reach - lengths[sink]) // 2
    margin = jnp.where((giver == sequence[0]) | (sink == sequence[0]) | (lengths[sink] == 0), 0, jnp.maximum(margin, 0))
    shifted = jax.random.randint(jax.random.fold_in(own, 4), (count // 2,), 0, 1 << 20) % (margin + 1)
    lengths = lengths.at[giver].add(-shifted).at[sink].add(shifted)
    items = jnp.searchsorted(jnp.cumsum(lengths), jnp.arange(rows * top), side="right").astype(jnp.int32)
    listing = items.reshape(top, rows).T
    listing = listing[jax.random.permutation(jax.random.fold_in(own, 1), rows)]
    turn = jax.random.randint(jax.random.fold_in(own, 2), (rows, 1), 0, top)
    return jnp.take_along_axis(listing, (jnp.arange(top)[None, :] + turn) % top, axis=1)


def shares(number_of, total, most, skew, full):
    loads = [(1 << 20) // math.isqrt(standing ** skew) + 1 for standing in range(1, number_of + 1)]
    largest = most if full else min(most, max(-(-total // number_of), total * loads[0] // sum(loads)))
    least = 1 if total - largest >= number_of - 1 else 0
    counts, surplus = [largest] + [least] * (number_of - 1), total - largest - least * (number_of - 1)
    while surplus > 0:
        movable = [i for i in range(1, number_of) if counts[i] < largest] or [i for i in range(1, number_of) if counts[i] < most]
        pool, budget = sum([loads[i] for i in movable]), surplus
        for i in movable:
            more = min(most - counts[i], max(1, budget * loads[i] // pool), surplus)
            counts[i] = counts[i] + more
            surplus = surplus - more
    return np.array(counts)


def bell_draw(stream_key, extent, width, bound, cuts=(), held_as=jnp.bfloat16):
    values = width * jax.random.normal(stream_key, extent, jnp.float32)
    if cuts:
        values = values * level_of(stream_key, extent, cuts, -0.22, 0.18)
    return jnp.clip(values, -bound, bound).astype(held_as)


def setup_inputs(seed: int = 0) -> dict:
    arg_keys = jax.random.split(jax.random.key(seed), 7)
    object_field = bell_draw(arg_keys[0], (2, OBJ_ROWS, OBJ_COLS), 1.0, 6.0, ((1, 8), (2, 4)), jnp.float32)
    probe = bell_draw(arg_keys[1], (MODES, 2, FRAME, FRAME), 1.0, 6.0, (), jnp.float32)
    raw_counts = jnp.clip(jnp.exp(math.log(10.0) - 4.609084 * jax.random.uniform(arg_keys[2], (FRAMES, FRAME, FRAME), jnp.float32) ** level_of(arg_keys[2], (FRAMES, FRAME, FRAME), ((0, 32),), -0.2, 0.2)), 0.099609375, 10.0).astype(jnp.bfloat16)
    resample_delta = bell_draw(arg_keys[3], (FRAME, FRAME), (4 * FRAME) ** -0.5, 0.1875, (), jnp.float32)
    tile_row_keys = jax.random.split(jax.random.fold_in(arg_keys[4], 1), FRAMES // FR_DEV)
    tile_row_turns = jax.random.permutation(jax.random.fold_in(arg_keys[4], 3), FRAMES // FR_DEV)
    tile_row = jax.vmap(lambda own, number: shared_out(jax.random.fold_in(arg_keys[4], 2), own, number, FR_DEV, N_ROW, 1, 1, 2))(tile_row_keys, tile_row_turns).reshape((FRAMES, 1))
    offsets = set_ends(jax.random.randint(arg_keys[5], (FRAMES, 2), 0, TILE), jax.random.fold_in(arg_keys[5], 1), 0, TILE - 1).astype(jnp.int32)
    return {"object_field": object_field, "probe": probe, "raw_counts": raw_counts, "resample_delta": resample_delta, "tile_row": tile_row, "offsets": offsets}


def product(left, right):
    return jnp.dot(left.astype(jnp.float32), right.astype(jnp.float32), preferred_element_type=jnp.float32)

def dft_tables(points):
    indices = jnp.arange(points, dtype=jnp.int32)
    phases = indices[:, None] * indices[None, :] % points
    angles = phases.astype(jnp.float32) * (2.0 * math.pi / points)
    norming = 1.0 / math.sqrt(points)
    cosine = jnp.cos(angles) * norming
    sine_part = -jnp.sin(angles) * norming
    forward = jnp.concatenate([jnp.concatenate([cosine, -sine_part], 1), jnp.concatenate([sine_part, cosine], 1)], 0)
    backward = jnp.concatenate([jnp.concatenate([cosine, sine_part], 1), jnp.concatenate([-sine_part, cosine], 1)], 0)
    return (forward.astype(jnp.bfloat16), backward.astype(jnp.bfloat16))

def measure(raw_counts, resample_delta):
    points = resample_delta.shape[0]
    resample = (jnp.eye(points, dtype=jnp.float32) + resample_delta).astype(jnp.bfloat16)
    first = jnp.einsum('ij,kjl->kil', resample.astype(jnp.float32), raw_counts.astype(jnp.float32)).astype(jnp.bfloat16)
    second = jnp.einsum('kij,lj->kil', first.astype(jnp.float32), resample.astype(jnp.float32))
    return jnp.sqrt(jnp.maximum(second, 0.0)).astype(jnp.bfloat16)

def frame_terms(window, probe, amplitude, forward, backward):
    mode_count = probe.shape[0]
    points = probe.shape[-1]
    probe_real = probe[:, 0]
    probe_imag = probe[:, 1]
    object_real = window[0]
    object_imag = window[1]
    wave = jnp.stack([probe_real * object_real - probe_imag * object_imag, probe_real * object_imag + probe_imag * object_real], 1)
    wave_cols = wave.transpose(1, 2, 0, 3).reshape(2 * points, mode_count * points).astype(jnp.bfloat16)
    half_done = product(forward, wave_cols).astype(jnp.bfloat16)
    wave_rows = half_done.reshape(2, points, mode_count, points).transpose(2, 1, 0, 3).reshape(mode_count * points, 2 * points)
    far_field = product(wave_rows, backward).reshape(mode_count, points, 2, points)
    intensity = lax.optimization_barrier(jnp.sum(far_field * far_field, axis=(0, 2)))
    scaling = 1.0 - amplitude.astype(jnp.float32) / jnp.sqrt(jnp.maximum(intensity, 1.0))
    residual = (far_field * scaling[None, :, None, :]).astype(jnp.bfloat16).reshape(mode_count * points, 2 * points)
    back_rows = product(residual, forward).astype(jnp.bfloat16)
    back_cols = back_rows.reshape(mode_count, points, 2, points).transpose(2, 1, 0, 3).reshape(2 * points, mode_count * points)
    update = product(backward, back_cols).reshape(2, points, mode_count, points).transpose(2, 0, 1, 3)
    update_real = update[:, 0]
    update_imag = update[:, 1]
    object_term = jnp.stack([lax.optimization_barrier(jnp.sum(probe_real * update_real + probe_imag * update_imag, 0)), lax.optimization_barrier(jnp.sum(probe_real * update_imag - probe_imag * update_real, 0))], 0)
    probe_term = jnp.stack([object_real * update_real + object_imag * update_imag, object_real * update_imag - object_imag * update_real], 1)
    return (object_term, probe_term)

def reference(object_field, probe, raw_counts, resample_delta, tile_row, offsets):
    points = probe.shape[-1]
    half = points // 2
    forward, backward = dft_tables(points)
    amplitudes = measure(raw_counts, resample_delta)
    padded = jnp.pad(object_field, ((0, 0), (half, half), (half, half)))
    frame_ids = jnp.arange(FRAMES, dtype=jnp.int32)
    tile_cols = frame_ids // FR_DEV % N_COL
    tops = (tile_row[:, 0] * TILE + offsets[:, 0]).astype(jnp.int32)
    lefts = (tile_cols * TILE + offsets[:, 1]).astype(jnp.int32)
    anchor = jnp.zeros((), jnp.int32)

    def one_frame(totals, inputs):
        gradient, probe_total = totals
        amplitude, top, left = inputs
        window = lax.dynamic_slice(padded, (anchor, top, left), (2, points, points))
        object_term, probe_term = frame_terms(window, probe, amplitude, forward, backward)
        current = lax.dynamic_slice(gradient, (anchor, top, left), (2, points, points))
        gradient = lax.dynamic_update_slice(gradient, current + object_term, (anchor, top, left))
        return ((gradient, probe_total + probe_term), None)
    start = (jnp.zeros(padded.shape, padded.dtype), jnp.zeros(probe.shape, probe.dtype))
    (gradient, probe_total), _ = lax.scan(one_frame, start, (amplitudes, tops, lefts))
    object_grad = gradient[:, half:half + OBJ_ROWS, half:half + OBJ_COLS]
    probe_grad = probe_total * (1.0 / math.sqrt(FRAMES))
    return (object_grad, probe_grad)
```

```python
import math

import jax
import jax.numpy as jnp
from jax import lax
from jax.experimental import pallas as pl
from jax.experimental.pallas import tpu as pltpu
from jax.sharding import PartitionSpec as P


MESH = pl.DeviceIdType.MESH
DIRECTIONS = tuple(
    (down, across) for down in (-1, 0, 1) for across in (-1, 0, 1) if (down, across) != (0, 0)
)


def place():
    return (
        lax.axis_index("row"),
        lax.axis_index("col"),
        lax.axis_size("row"),
        lax.axis_size("col"),
    )


def inside(row, col, rows, cols):
    return (row >= 0) & (row < rows) & (col >= 0) & (col < cols)


def inner_edge(step, tile, half):
    start, size = {-1: (0, half), 0: (0, tile), 1: (tile - half, half)}[step]
    return pl.ds(start, size)


def outer_edge(step, tile, half):
    start, size = {-1: (0, half), 0: (half, tile), 1: (half + tile, half)}[step]
    return pl.ds(start, size)


def greet(pair):
    row, col, rows, cols = place()
    barrier = pltpu.get_barrier_semaphore()
    others = [(lax.rem(row + i, rows), col) for i in range(1, rows)]
    if pair:
        others += [(row, lax.rem(col + i, cols)) for i in range(1, cols)]
    else:
        others += [(row, lax.rem(col + i, cols)) for i in (1, cols - 1)]
    for down in (1, rows - 1):
        for across in (1, cols - 1):
            others.append((lax.rem(row + down, rows), lax.rem(col + across, cols)))
    for other in others:
        pl.semaphore_signal(barrier, inc=1, device_id=other, device_id_type=MESH)
    pl.semaphore_wait(barrier, len(others))


def gather_kernel(
    tile_row,
    offsets,
    object_field,
    raw_counts,
    delta,
    extended,
    incoming,
    infos,
    outbox,
    info_out,
    halo_send,
    halo_recv,
    slot_send,
    slot_recv,
    info_send,
    info_recv,
    center_sem,
):
    row, col, rows, cols = place()
    tile = object_field.shape[1]
    points = raw_counts.shape[1]
    half = points // 2
    frame_count = raw_counts.shape[0]
    center = pltpu.make_async_copy(
        object_field, extended.at[:, pl.ds(half, tile), pl.ds(half, tile)], center_sem
    )
    center.start()
    greet(False)

    def halo(index):
        down, across = DIRECTIONS[index]
        return pltpu.make_async_remote_copy(
            src_ref=object_field.at[
                :, inner_edge(down, tile, half), inner_edge(across, tile, half)
            ],
            dst_ref=extended.at[
                :, outer_edge(-down, tile, half), outer_edge(-across, tile, half)
            ],
            send_sem=halo_send.at[index],
            recv_sem=halo_recv.at[index],
            device_id=(row + down, col + across),
            device_id_type=MESH,
        )

    for index, (down, across) in enumerate(DIRECTIONS):

        @pl.when(inside(row + down, col + across, rows, cols))
        def _():
            halo(index).start()

        @pl.when(jnp.logical_not(inside(row - down, col - across, rows, cols)))
        def _():
            where = (slice(None), outer_edge(-down, tile, half), outer_edge(-across, tile, half))
            extended[where] = jnp.zeros(
                (2, where[1].size, where[2].size), jnp.float32
            )

    identity = (
        lax.broadcasted_iota(jnp.int32, (points, points), 0)
        == lax.broadcasted_iota(jnp.int32, (points, points), 1)
    ).astype(jnp.float32)
    resample = (identity + delta[...]).astype(jnp.bfloat16)

    def slot(step):
        other = lax.rem(row + step, rows)
        return (
            pltpu.make_async_remote_copy(
                src_ref=outbox.at[step],
                dst_ref=incoming.at[row],
                send_sem=slot_send.at[step],
                recv_sem=slot_recv.at[row],
                device_id=(other, col),
                device_id_type=MESH,
            ),
            pltpu.make_async_remote_copy(
                src_ref=info_out.at[step],
                dst_ref=infos.at[row],
                send_sem=info_send.at[step],
                recv_sem=info_recv.at[row],
                device_id=(other, col),
                device_id_type=MESH,
            ),
        )

    lanes = lax.broadcasted_iota(jnp.int32, (8, 128), 1)

    def fill(step, carry):
        other = lax.rem(row + step, rows)
        pick, top, left, live = (jnp.int32(0), jnp.int32(0), jnp.int32(0), jnp.int32(0))
        for k in range(frame_count):
            hit = tile_row[k, 0] == other
            pick = jnp.where(hit, k, pick)
            top = jnp.where(hit, offsets[k, 0], top)
            left = jnp.where(hit, offsets[k, 1], left)
            live = jnp.where(hit, 1, live)
        info = jnp.where(lanes == 0, top, jnp.where(lanes == 1, left, live))
        first = product(resample, raw_counts[pick]).astype(jnp.bfloat16)
        second = lax.dot_general(
            first, resample, (((1,), (1,)), ((), ())), preferred_element_type=jnp.float32
        )
        amplitude = jnp.sqrt(jnp.maximum(second, 0.0)).astype(jnp.bfloat16)

        @pl.when(step == 0)
        def _():
            incoming[row] = amplitude
            infos[row] = info

        @pl.when(step > 0)
        def _():
            outbox[step] = amplitude
            info_out[step] = info
            for copy in slot(step):
                copy.start()

        return carry

    lax.fori_loop(0, rows, fill, 0)

    for index, (down, across) in enumerate(DIRECTIONS):

        @pl.when(inside(row - down, col - across, rows, cols))
        def _():
            halo(index).wait_recv()

        @pl.when(inside(row + down, col + across, rows, cols))
        def _():
            halo(index).wait_send()

    center.wait()

    def finish(step, carry):
        source = lax.rem(row + step, rows)
        pltpu.make_async_remote_copy(
            src_ref=outbox.at[step],
            dst_ref=incoming.at[source],
            send_sem=slot_send.at[step],
            recv_sem=slot_recv.at[source],
            device_id=(source, col),
            device_id_type=MESH,
        ).wait()
        pltpu.make_async_remote_copy(
            src_ref=info_out.at[step],
            dst_ref=infos.at[source],
            send_sem=info_send.at[step],
            recv_sem=info_recv.at[source],
            device_id=(source, col),
            device_id_type=MESH,
        ).wait()
        return carry

    lax.fori_loop(1, rows, finish, 0)


def gather(tile_row, offsets, object_field, raw_counts, delta):
    rows = lax.axis_size("row")
    points = raw_counts.shape[1]
    reach = object_field.shape[1] + points
    vmem = pl.BlockSpec(memory_space=pltpu.VMEM)
    smem = pl.BlockSpec(memory_space=pltpu.SMEM)
    dma = pltpu.SemaphoreType.DMA
    return pl.pallas_call(
        gather_kernel,
        name="gather",
        out_shape=(
            jax.ShapeDtypeStruct((2, reach, reach), jnp.float32),
            jax.ShapeDtypeStruct((rows, points, points), jnp.bfloat16),
            jax.ShapeDtypeStruct((rows, 8, 128), jnp.int32),
        ),
        in_specs=[smem, smem, pl.BlockSpec(memory_space=pl.ANY), vmem, vmem],
        out_specs=(vmem, vmem, vmem),
        scratch_shapes=[
            pltpu.VMEM((rows, points, points), jnp.bfloat16),
            pltpu.VMEM((rows, 8, 128), jnp.int32),
            dma((8,)),
            dma((8,)),
            dma((rows,)),
            dma((rows,)),
            dma((rows,)),
            dma((rows,)),
            dma,
        ],
        compiler_params=pltpu.CompilerParams(
            collective_id=0, has_side_effects=True, vmem_limit_bytes=40 * 1024 * 1024
        ),
    )(tile_row, offsets, object_field, raw_counts, delta)


def scatter_kernel(
    gradient,
    total,
    folded,
    summed,
    halos_tall,
    halos_wide,
    corners,
    pair_in,
    pair_sum,
    chip_in,
    chip_sum,
    line_in,
    line_sum,
    line_out,
    chip_out,
    halo_send,
    halo_recv,
    pair_sems,
    chip_sems,
    line_sems,
    back_line_sems,
    back_chip_sems,
    back_pair_sems,
):
    row, col, rows, cols = place()
    tile = folded.shape[1]
    half = (gradient.shape[1] - tile) // 2
    pieces = pair_in.shape[0]
    length = pair_in.shape[1]
    chips = rows // 2
    core, chip = (lax.rem(row, 2), row // 2)
    chip_rows = length // chips
    line_rows = chip_rows // cols
    lanes = summed.shape[2] // 2

    def own_half():
        return pl.ds(pl.multiple_of(core * lanes, lanes), lanes)

    def sibling_half():
        return pl.ds(pl.multiple_of((1 - core) * lanes, lanes), lanes)

    sibling = (row + 1 - 2 * core, col)
    greet(True)

    def landing(index):
        down, across = DIRECTIONS[index]
        if down and across:
            return corners.at[(down + 1) + (across + 1) // 2]
        return halos_wide.at[(down + 1) // 2] if down else halos_tall.at[(across + 1) // 2]

    def halo(index):
        down, across = DIRECTIONS[index]
        return pltpu.make_async_remote_copy(
            src_ref=gradient.at[:, outer_edge(down, tile, half), outer_edge(across, tile, half)],
            dst_ref=landing(index),
            send_sem=halo_send.at[index],
            recv_sem=halo_recv.at[index],
            device_id=(row + down, col + across),
            device_id_type=MESH,
        )

    def start_halo(index):
        down, across = DIRECTIONS[index]

        @pl.when(inside(row + down, col + across, rows, cols))
        def _():
            halo(index).start()

    def remote(source, target, sems, index, device):
        return pltpu.make_async_remote_copy(
            src_ref=source,
            dst_ref=target,
            send_sem=sems.at[0, index],
            recv_sem=sems.at[1, index],
            device_id=device,
            device_id_type=MESH,
        )

    def pair_copy(piece):
        return remote(
            total.at[piece, :, sibling_half()], pair_in.at[piece], pair_sems, piece, sibling
        )

    def chip_copy(piece, step):
        other = lax.rem(chip + step, chips)
        start = pl.multiple_of(other * chip_rows, 8)
        index = piece * chips + step
        return remote(
            pair_sum.at[piece, pl.ds(start, chip_rows)],
            chip_in.at[index],
            chip_sems,
            index,
            (2 * other + core, col),
        )

    def line_copy(piece, step):
        other = lax.rem(col + step, cols)
        start = pl.multiple_of(other * line_rows, 8)
        index = piece * cols + step
        return remote(
            chip_sum.at[piece, pl.ds(start, line_rows)],
            line_in.at[index],
            line_sems,
            index,
            (row, other),
        )

    def back_line_copy(piece, step):
        other = lax.rem(col + step, cols)
        start = pl.multiple_of(col * line_rows, 8)
        return remote(
            line_sum.at[piece],
            line_out.at[piece, pl.ds(start, line_rows)],
            back_line_sems,
            piece * cols + step,
            (row, other),
        )

    def back_chip_copy(piece, step):
        other = lax.rem(chip + step, chips)
        start = pl.multiple_of(chip * chip_rows, 8)
        return remote(
            line_out.at[piece],
            chip_out.at[piece, pl.ds(start, chip_rows)],
            back_chip_sems,
            piece * chips + step,
            (2 * other + core, col),
        )

    def back_pair_copy(piece):
        return remote(
            chip_out.at[piece],
            summed.at[piece, :, own_half()],
            back_pair_sems,
            piece,
            sibling,
        )

    for piece in range(pieces):
        pair_copy(piece).start()
    for index, (down, across) in enumerate(DIRECTIONS):
        if not down:
            start_halo(index)
    for piece in range(pieces):
        pair_copy(piece).wait_recv()
        pair_sum[piece] = total[piece, :, own_half()] + pair_in[piece]
        for step in range(1, chips):
            chip_copy(piece, step).start()
    for index, (down, across) in enumerate(DIRECTIONS):
        if down:
            start_halo(index)
    for piece in range(pieces):
        start = pl.multiple_of(chip * chip_rows, 8)
        value = pair_sum[piece, pl.ds(start, chip_rows)]
        for step in range(1, chips):
            chip_copy(piece, step).wait_recv()
            value = value + chip_in[piece * chips + step]
        chip_sum[piece] = value
        for step in range(1, cols):
            line_copy(piece, step).start()
    for piece in range(pieces):
        start = pl.multiple_of(col * line_rows, 8)
        value = chip_sum[piece, pl.ds(start, line_rows)]
        for step in range(1, cols):
            line_copy(piece, step).wait_recv()
            value = value + line_in[piece * cols + step]
        line_sum[piece] = value
        line_out[piece, pl.ds(start, line_rows)] = value
        for step in range(1, cols):
            back_line_copy(piece, step).start()
    for piece in range(pieces):
        for step in range(1, cols):
            back_line_copy(piece, step).wait_recv()
        start = pl.multiple_of(chip * chip_rows, 8)
        for step in range(1, chips):
            back_chip_copy(piece, step).start()
        chip_out[piece, pl.ds(start, chip_rows)] = line_out[piece]
    for piece in range(pieces):
        for step in range(1, chips):
            back_chip_copy(piece, step).wait_recv()
        back_pair_copy(piece).start()
        summed[piece, :, own_half()] = chip_out[piece]

    folded[...] = gradient[:, half : half + tile, half : half + tile]
    for index, (down, across) in enumerate(DIRECTIONS):

        @pl.when(inside(row - down, col - across, rows, cols))
        def _():
            halo(index).wait_recv()
            where = (slice(None), inner_edge(-down, tile, half), inner_edge(-across, tile, half))
            folded[where] += landing(index)[...]

    for piece in range(pieces):
        back_pair_copy(piece).wait_recv()
    for index, (down, across) in enumerate(DIRECTIONS):

        @pl.when(inside(row + down, col + across, rows, cols))
        def _():
            halo(index).wait_send()

    for piece in range(pieces):
        pair_copy(piece).wait_send()
        back_pair_copy(piece).wait_send()
        for step in range(1, chips):
            chip_copy(piece, step).wait_send()
            back_chip_copy(piece, step).wait_send()
        for step in range(1, cols):
            line_copy(piece, step).wait_send()
            back_line_copy(piece, step).wait_send()


def scatter(gradient, total, tile):
    rows, cols = (lax.axis_size("row"), lax.axis_size("col"))
    half = (gradient.shape[1] - tile) // 2
    pieces, _, points, _ = total.shape
    length, lanes = (2 * points, points // 2)
    chips = rows // 2
    f32 = jnp.float32
    vmem = pl.BlockSpec(memory_space=pltpu.VMEM)
    dma = pltpu.SemaphoreType.DMA
    folded, summed = pl.pallas_call(
        scatter_kernel,
        name="scatter",
        out_shape=(
            jax.ShapeDtypeStruct((2, tile, tile), f32),
            jax.ShapeDtypeStruct((pieces, length, points), f32),
        ),
        in_specs=[vmem, vmem],
        out_specs=(vmem, vmem),
        scratch_shapes=[
            pltpu.VMEM((2, 2, tile, half), f32),
            pltpu.VMEM((2, 2, half, tile), f32),
            pltpu.VMEM((4, 2, half, half), f32),
            pltpu.VMEM((pieces, length, lanes), f32),
            pltpu.VMEM((pieces, length, lanes), f32),
            pltpu.VMEM((pieces * chips, length // chips, lanes), f32),
            pltpu.VMEM((pieces, length // chips, lanes), f32),
            pltpu.VMEM((pieces * cols, length // chips // cols, lanes), f32),
            pltpu.VMEM((pieces, length // chips // cols, lanes), f32),
            pltpu.VMEM((pieces, length // chips, lanes), f32),
            pltpu.VMEM((pieces, length, lanes), f32),
            dma((8,)),
            dma((8,)),
            dma((2, pieces)),
            dma((2, pieces * chips)),
            dma((2, pieces * cols)),
            dma((2, pieces * cols)),
            dma((2, pieces * chips)),
            dma((2, pieces)),
        ],
        compiler_params=pltpu.CompilerParams(
            collective_id=1, has_side_effects=True, vmem_limit_bytes=40 * 1024 * 1024
        ),
    )(gradient, total.reshape(pieces, length, points))
    return folded, summed.reshape(total.shape)


def product(left, right):
    return jnp.dot(left, right, preferred_element_type=jnp.float32)


def dft_tables(points):
    indices = jnp.arange(points, dtype=jnp.int32)
    phases = indices[:, None] * indices[None, :] % points
    angles = phases.astype(jnp.float32) * (2.0 * math.pi / points)
    norming = 1.0 / math.sqrt(points)
    cosine = jnp.cos(angles) * norming
    sine_part = -jnp.sin(angles) * norming
    forward = jnp.concatenate(
        [jnp.concatenate([cosine, -sine_part], 1), jnp.concatenate([sine_part, cosine], 1)], 0
    )
    backward = jnp.concatenate(
        [jnp.concatenate([cosine, sine_part], 1), jnp.concatenate([-sine_part, cosine], 1)], 0
    )
    return (forward.astype(jnp.bfloat16), backward.astype(jnp.bfloat16))


def frames_kernel(
    requests,
    extended,
    probe,
    amplitudes,
    forward,
    backward,
    gradient,
    probe_total,
    window,
    far_field,
):
    mode_count, _, points, _ = probe.shape
    span_rows, span_cols = (points + 8, points + 128)
    gradient[...] = jnp.zeros_like(gradient)
    probe_total[...] = jnp.zeros_like(probe_total)

    def one_slot(slot, carry):
        @pl.when(requests[slot, 2] > 0)
        def _():
            top, left = (requests[slot, 0], requests[slot, 1])
            skip_rows, skip_cols = (lax.rem(top, 8), lax.rem(left, 128))
            rows = pl.ds(pl.multiple_of(top - skip_rows, 8), span_rows)
            cols = pl.ds(pl.multiple_of(left - skip_cols, 128), span_cols)
            for part in range(2):
                block = extended[part, rows, cols]
                block = pltpu.roll(block, lax.rem(span_cols - skip_cols, span_cols), 1)
                block = block[:, :points]
                block = pltpu.roll(block, lax.rem(span_rows - skip_rows, span_rows), 0)
                window[part] = block[:points]
            intensity = jnp.zeros((points, points), jnp.float32)
            for mode in range(mode_count):
                object_real, object_imag = (window[0], window[1])
                probe_real, probe_imag = (probe[mode, 0], probe[mode, 1])
                wave = jnp.concatenate(
                    [
                        (probe_real * object_real - probe_imag * object_imag).astype(jnp.bfloat16),
                        (probe_real * object_imag + probe_imag * object_real).astype(jnp.bfloat16),
                    ],
                    0,
                )
                half_done = product(forward[...], wave).astype(jnp.bfloat16)
                wave_rows = jnp.concatenate([half_done[:points], half_done[points:]], 1)
                field = product(wave_rows, backward[...])
                far_field[mode] = field
                squares = field * field
                intensity = intensity + squares[:, :points] + squares[:, points:]
            amplitude = amplitudes[slot].astype(jnp.float32)
            scaling = 1.0 - amplitude / jnp.sqrt(jnp.maximum(intensity, 1.0))
            scaling = jnp.concatenate([scaling, scaling], 1)
            term_real = jnp.zeros((points, points), jnp.float32)
            term_imag = jnp.zeros((points, points), jnp.float32)
            for mode in range(mode_count):
                residual = (far_field[mode] * scaling).astype(jnp.bfloat16)
                back_rows = product(residual, forward[...]).astype(jnp.bfloat16)
                back_cols = jnp.concatenate([back_rows[:, :points], back_rows[:, points:]], 0)
                update = product(backward[...], back_cols)
                update_real, update_imag = (update[:points], update[points:])
                object_real, object_imag = (window[0], window[1])
                probe_real, probe_imag = (probe[mode, 0], probe[mode, 1])
                term_real = term_real + (probe_real * update_real + probe_imag * update_imag)
                term_imag = term_imag + (probe_real * update_imag - probe_imag * update_real)
                probe_total[mode, 0] += object_real * update_real + object_imag * update_imag
                probe_total[mode, 1] += object_real * update_imag - object_imag * update_real
            for part, term in enumerate((term_real, term_imag)):
                block = jnp.concatenate([term, jnp.zeros((8, points), jnp.float32)], 0)
                block = pltpu.roll(block, skip_rows, 0)
                block = jnp.concatenate([block, jnp.zeros((span_rows, 128), jnp.float32)], 1)
                block = pltpu.roll(block, skip_cols, 1)
                gradient[part, rows, cols] += block

        return carry

    lax.fori_loop(0, requests.shape[0], one_slot, 0)


def frames(requests, extended, probe, amplitudes, forward, backward):
    points = probe.shape[-1]
    vmem = pl.BlockSpec(memory_space=pltpu.VMEM)
    return pl.pallas_call(
        frames_kernel,
        name="frames",
        out_shape=(
            jax.ShapeDtypeStruct(extended.shape, jnp.float32),
            jax.ShapeDtypeStruct(probe.shape, jnp.float32),
        ),
        in_specs=[pl.BlockSpec(memory_space=pltpu.SMEM)] + [vmem] * 5,
        out_specs=(vmem, vmem),
        scratch_shapes=[
            pltpu.VMEM((2, points, points), jnp.float32),
            pltpu.VMEM((probe.shape[0], points, 2 * points), jnp.float32),
        ],
        compiler_params=pltpu.CompilerParams(vmem_limit_bytes=48 * 1024 * 1024),
    )(requests, extended, probe, amplitudes, forward, backward)


def shards(object_field, probe, raw_counts, resample_delta, tile_row, offsets):
    points = probe.shape[-1]
    tile = object_field.shape[1]
    frame_total = raw_counts.shape[0] * lax.axis_size("row") * lax.axis_size("col")
    forward, backward = dft_tables(points)
    extended, incoming, infos = gather(
        tile_row, offsets, object_field, raw_counts, resample_delta
    )
    requests = infos[:, 0, :3]
    gradient, probe_total = frames(requests, extended, probe, incoming, forward, backward)
    object_grad, summed = scatter(gradient, probe_total, tile)
    return (object_grad, summed * (1.0 / math.sqrt(frame_total)))


def solution(mesh):
    placed = (
        P(None, "row", "col"),
        P(),
        P(("row", "col"), None, None),
        P(),
        P(("row", "col"), None),
        P(("row", "col"), None),
    )
    return jax.shard_map(
        shards, mesh=mesh, in_specs=placed, out_specs=(P(None, "row", "col"), P()), check_vma=False
    )
```

```python
import math

import jax
import jax.numpy as jnp
import numpy as np
from jax import lax
from jax.experimental import pallas as pl
from jax.experimental.pallas import tpu as pltpu
from jax.sharding import PartitionSpec as P


MESH = pl.DeviceIdType.MESH
DIRECTIONS = tuple(
    (down, across) for down in (-1, 0, 1) for across in (-1, 0, 1) if (down, across) != (0, 0)
)


def place():
    return (
        lax.axis_index("row"),
        lax.axis_index("col"),
        lax.axis_size("row"),
        lax.axis_size("col"),
    )


def inside(row, col, rows, cols):
    return (row >= 0) & (row < rows) & (col >= 0) & (col < cols)


def inner_edge(step, tile, half):
    start, size = {-1: (0, half), 0: (0, tile), 1: (tile - half, half)}[step]
    return pl.ds(start, size)


def outer_edge(step, tile, half):
    start, size = {-1: (0, half), 0: (half, tile), 1: (half + tile, half)}[step]
    return pl.ds(start, size)


def greet():
    row, col, rows, cols = place()
    barrier = pltpu.get_barrier_semaphore()
    others = [(lax.rem(row + i, rows), col) for i in range(1, rows)]
    others += [(row, lax.rem(col + i, cols)) for i in range(1, cols)]
    for down in (1, rows - 1):
        for across in (1, cols - 1):
            others.append((lax.rem(row + down, rows), lax.rem(col + across, cols)))
    for other in others:
        pl.semaphore_signal(barrier, inc=1, device_id=other, device_id_type=MESH)
    pl.semaphore_wait(barrier, len(others))


def product(left, right):
    return jnp.dot(left, right, preferred_element_type=jnp.float32)


def dft_tables(points):
    indices = np.arange(points)
    angles = (indices[:, None] * indices[None, :] % points) * (2.0 * math.pi / points)
    cosine = np.cos(angles) / math.sqrt(points)
    sine_part = -np.sin(angles) / math.sqrt(points)
    forward = np.block([[cosine, -sine_part], [sine_part, cosine]])
    backward = np.block([[cosine, sine_part], [-sine_part, cosine]])
    return (jnp.asarray(forward, jnp.bfloat16), jnp.asarray(backward, jnp.bfloat16))


def whole_kernel(
    table,
    object_hbm,
    probe_hbm,
    raw_hbm,
    delta_hbm,
    forward_hbm,
    backward_hbm,
    folded,
    summed,
    probe,
    raw,
    delta,
    forward,
    backward,
    extended,
    incoming,
    outbox,
    infos,
    info_out,
    places,
    windows,
    residuals,
    far_field,
    terms,
    total,
    shifted,
    halos_tall,
    halos_wide,
    corners,
    pair_in,
    pair_sum,
    chip_in,
    chip_sum,
    line_in,
    line_sum,
    line_out,
    chip_out,
    local_sems,
    object_send,
    object_recv,
    slot_send,
    slot_recv,
    info_send,
    info_recv,
    halo_send,
    halo_recv,
    pair_sems,
    chip_sems,
    line_sems,
    back_line_sems,
    back_chip_sems,
    back_pair_sems,
):
    row, col, rows, cols = place()
    tile = folded.shape[1]
    points = raw.shape[1]
    half = points // 2
    reach = tile + points
    mode_count = probe.shape[0]
    frame_count = raw.shape[0]
    gradient = extended

    loads = [
        pltpu.make_async_copy(source, target, local_sems.at[i])
        for i, (source, target) in enumerate(
            (
                (raw_hbm, raw),
                (delta_hbm, delta),
                (object_hbm, extended.at[:, pl.ds(half, tile), pl.ds(half, tile)]),
                (probe_hbm, probe),
                (forward_hbm, forward),
                (backward_hbm, backward),
            )
        )
    ]
    for load in loads:
        load.start()
    greet()

    lanes_of = lax.broadcasted_iota(jnp.int32, (8, 128), 1)

    def chosen(other):
        pick, top, left, live = (jnp.int32(0), jnp.int32(0), jnp.int32(0), jnp.int32(0))
        for k in range(frame_count):
            hit = table[k, 0] == other
            pick = jnp.where(hit, k, pick)
            top = jnp.where(hit, table[k, 1], top)
            left = jnp.where(hit, table[k, 2], left)
            live = jnp.where(hit, 1, live)
        return pick, top, left, live

    def info_copy(step, target, other):
        return pltpu.make_async_remote_copy(
            src_ref=info_out.at[step],
            dst_ref=infos.at[target],
            send_sem=info_send.at[step],
            recv_sem=info_recv.at[target],
            device_id=(other, col),
            device_id_type=MESH,
        )

    def slot_copy(step, target, other):
        return pltpu.make_async_remote_copy(
            src_ref=outbox.at[step],
            dst_ref=incoming.at[target],
            send_sem=slot_send.at[step],
            recv_sem=slot_recv.at[target],
            device_id=(other, col),
            device_id_type=MESH,
        )

    def tell(step, carry):
        other = lax.rem(row + step, rows)
        _, top, left, live = chosen(other)
        info = jnp.where(lanes_of == 0, top, jnp.where(lanes_of == 1, left, live))

        @pl.when(step == 0)
        def _():
            infos[row] = info

        @pl.when(step > 0)
        def _():
            info_out[step] = info
            info_copy(step, row, other).start()

        return carry

    lax.fori_loop(0, rows, tell, 0)

    def object_halo(index):
        down, across = DIRECTIONS[index]
        return pltpu.make_async_remote_copy(
            src_ref=object_hbm.at[
                :, inner_edge(down, tile, half), inner_edge(across, tile, half)
            ],
            dst_ref=extended.at[
                :, outer_edge(-down, tile, half), outer_edge(-across, tile, half)
            ],
            send_sem=object_send.at[index],
            recv_sem=object_recv.at[index],
            device_id=(row + down, col + across),
            device_id_type=MESH,
        )

    for index, (down, across) in enumerate(DIRECTIONS):

        @pl.when(inside(row + down, col + across, rows, cols))
        def _():
            object_halo(index).start()

        @pl.when(jnp.logical_not(inside(row - down, col - across, rows, cols)))
        def _():
            where = (slice(None), outer_edge(-down, tile, half), outer_edge(-across, tile, half))
            extended[where] = jnp.zeros((2, where[1].size, where[2].size), jnp.float32)

    loads[0].wait()
    loads[1].wait()
    identity = (
        lax.broadcasted_iota(jnp.int32, (points, points), 0)
        == lax.broadcasted_iota(jnp.int32, (points, points), 1)
    ).astype(jnp.float32)
    resample = (identity + delta[...]).astype(jnp.bfloat16)

    def measure(step, carry):
        other = lax.rem(row + step, rows)
        pick, _, _, _ = chosen(other)
        first = product(resample, raw[pick]).astype(jnp.bfloat16)
        second = lax.dot_general(
            first, resample, (((1,), (1,)), ((), ())), preferred_element_type=jnp.float32
        )
        amplitude = jnp.sqrt(jnp.maximum(second, 0.0)).astype(jnp.bfloat16)

        @pl.when(step == 0)
        def _():
            incoming[row] = amplitude

        @pl.when(step > 0)
        def _():
            outbox[step] = amplitude
            slot_copy(step, row, other).start()

        return carry

    lax.fori_loop(0, rows, measure, 0)

    def heard(step, carry):
        source = lax.rem(row - step + rows, rows)
        info_copy(step, source, source).wait()
        return carry

    lax.fori_loop(1, rows, heard, 0)
    noted = pltpu.make_async_copy(infos, places, local_sems.at[6])
    noted.start()
    total[...] = jnp.zeros_like(total)
    for load in loads[2:]:
        load.wait()
    noted.wait()
    for index, (down, across) in enumerate(DIRECTIONS):

        @pl.when(inside(row - down, col - across, rows, cols))
        def _():
            object_halo(index).wait_recv()

    span_rows, span_cols = (points + 8, points + 128)

    def spot(step):
        source = lax.rem(row - step + rows, rows)
        return source, places[source, 0, 0], places[source, 0, 1], places[source, 0, 2]

    def onward(step, carry):
        source, top, left, live = spot(step)
        skip_rows, skip_cols = (lax.rem(top, 8), lax.rem(left, 128))
        across_rows = pl.ds(lax.div(top, 8) * 8, span_rows)
        across_cols = pl.ds(lax.div(left, 128) * 128, span_cols)
        for part in range(2):
            block = extended[part, across_rows, across_cols]
            block = pltpu.roll(block, lax.rem(span_cols - skip_cols, span_cols), 1)
            block = block[:, :points]
            block = pltpu.roll(block, lax.rem(span_rows - skip_rows, span_rows), 0)
            windows[step, part] = block[:points]
        intensity = jnp.zeros((points, points), jnp.float32)
        for mode in range(mode_count):
            object_real, object_imag = (windows[step, 0], windows[step, 1])
            probe_real, probe_imag = (probe[mode, 0], probe[mode, 1])
            wave = jnp.concatenate(
                [
                    (probe_real * object_real - probe_imag * object_imag).astype(jnp.bfloat16),
                    (probe_real * object_imag + probe_imag * object_real).astype(jnp.bfloat16),
                ],
                0,
            )
            half_done = product(forward[...], wave).astype(jnp.bfloat16)
            wave_rows = jnp.concatenate([half_done[:points], half_done[points:]], 1)
            field = product(wave_rows, backward[...])
            far_field[mode] = field
            squares = field * field
            intensity = intensity + squares[:, :points] + squares[:, points:]

        @pl.when(step > 0)
        def _():
            slot_copy(step, source, source).wait_recv()

        amplitude = incoming[source].astype(jnp.float32)
        scaling = 1.0 - amplitude / jnp.sqrt(jnp.maximum(intensity, 1.0))
        scaling = scaling * live.astype(jnp.float32)
        scaling = jnp.concatenate([scaling, scaling], 1)
        for mode in range(mode_count):
            residuals[step, mode] = (far_field[mode] * scaling).astype(jnp.bfloat16)
        return carry

    lax.fori_loop(0, rows, onward, 0)

    def back(mode):
        def one(step, carry):
            back_rows = product(residuals[step, mode], forward[...]).astype(jnp.bfloat16)
            back_cols = jnp.concatenate([back_rows[:, :points], back_rows[:, points:]], 0)
            update = product(backward[...], back_cols)
            update_real, update_imag = (update[:points], update[points:])
            object_real, object_imag = (windows[step, 0], windows[step, 1])
            probe_real, probe_imag = (probe[mode, 0], probe[mode, 1])
            term_real = probe_real * update_real + probe_imag * update_imag
            term_imag = probe_real * update_imag - probe_imag * update_real
            if mode == 0:
                terms[step, 0] = term_real
                terms[step, 1] = term_imag
            else:
                terms[step, 0] += term_real
                terms[step, 1] += term_imag
            total[mode, :points] += object_real * update_real + object_imag * update_imag
            total[mode, points:] += object_real * update_imag - object_imag * update_real
            return carry

        return one

    def accumulate():
        gradient[...] = jnp.zeros_like(gradient)
        shifted[...] = jnp.zeros_like(shifted)
        chunk = 64

        def one(step, carry):
            _, top, left, _ = spot(step)
            skip_rows = lax.rem(top, 8)
            base = tile // 8 - lax.div(top, 8)
            for part in range(2):
                block = jnp.concatenate(
                    [terms[step, part], jnp.zeros((8, points), jnp.float32)], 0
                )
                block = pltpu.roll(block, skip_rows, 0)
                block = jnp.concatenate(
                    [block, jnp.zeros((span_rows, reach - points), jnp.float32)], 1
                )
                shifted[pl.ds(tile, span_rows)] = pltpu.roll(block, left, 1)

                def add(index, inner):
                    start = pl.multiple_of(index * chunk, 8)
                    source = (base + index * (chunk // 8)) * 8
                    gradient[part, pl.ds(start, chunk)] += shifted[pl.ds(source, chunk)]
                    return inner

                lax.fori_loop(0, reach // chunk, add, 0)
            return carry

        lax.fori_loop(0, rows, one, 0)

    pieces = pair_in.shape[0]
    length = pair_in.shape[1]
    chips = rows // 2
    core, chip = (lax.rem(row, 2), row // 2)
    chip_rows = length // chips
    line_rows = chip_rows // cols
    lanes = summed.shape[2] // 2

    def own_half():
        return pl.ds(pl.multiple_of(core * lanes, lanes), lanes)

    def sibling_half():
        return pl.ds(pl.multiple_of((1 - core) * lanes, lanes), lanes)

    sibling = (row + 1 - 2 * core, col)
    def landing(index):
        down, across = DIRECTIONS[index]
        if down and across:
            return corners.at[(down + 1) + (across + 1) // 2]
        return halos_wide.at[(down + 1) // 2] if down else halos_tall.at[(across + 1) // 2]

    def halo(index):
        down, across = DIRECTIONS[index]
        return pltpu.make_async_remote_copy(
            src_ref=gradient.at[:, outer_edge(down, tile, half), outer_edge(across, tile, half)],
            dst_ref=landing(index),
            send_sem=halo_send.at[index],
            recv_sem=halo_recv.at[index],
            device_id=(row + down, col + across),
            device_id_type=MESH,
        )

    def start_halo(index):
        down, across = DIRECTIONS[index]

        @pl.when(inside(row + down, col + across, rows, cols))
        def _():
            halo(index).start()

    def remote(source, target, sems, index, device):
        return pltpu.make_async_remote_copy(
            src_ref=source,
            dst_ref=target,
            send_sem=sems.at[0, index],
            recv_sem=sems.at[1, index],
            device_id=device,
            device_id_type=MESH,
        )

    def pair_copy(piece):
        return remote(
            total.at[piece, :, sibling_half()], pair_in.at[piece], pair_sems, piece, sibling
        )

    def chip_copy(piece, step):
        other = lax.rem(chip + step, chips)
        start = pl.multiple_of(other * chip_rows, 8)
        index = piece * chips + step
        return remote(
            pair_sum.at[piece, pl.ds(start, chip_rows)],
            chip_in.at[index],
            chip_sems,
            index,
            (2 * other + core, col),
        )

    def line_copy(piece, step):
        other = lax.rem(col + step, cols)
        start = pl.multiple_of(other * line_rows, 8)
        index = piece * cols + step
        return remote(
            chip_sum.at[piece, pl.ds(start, line_rows)],
            line_in.at[index],
            line_sems,
            index,
            (row, other),
        )

    def back_line_copy(piece, step):
        other = lax.rem(col + step, cols)
        start = pl.multiple_of(col * line_rows, 8)
        return remote(
            line_sum.at[piece],
            line_out.at[piece, pl.ds(start, line_rows)],
            back_line_sems,
            piece * cols + step,
            (row, other),
        )

    def back_chip_copy(piece, step):
        other = lax.rem(chip + step, chips)
        start = pl.multiple_of(chip * chip_rows, 8)
        return remote(
            line_out.at[piece],
            chip_out.at[piece, pl.ds(start, chip_rows)],
            back_chip_sems,
            piece * chips + step,
            (2 * other + core, col),
        )

    def back_pair_copy(piece):
        return remote(
            chip_out.at[piece],
            summed.at[piece, :, own_half()],
            back_pair_sems,
            piece,
            sibling,
        )

    def pair_stage(piece):
        pair_copy(piece).wait_recv()
        pair_sum[piece] = total[piece, :, own_half()] + pair_in[piece]
        for step in range(1, chips):
            chip_copy(piece, step).start()

    def chip_stage(piece):
        start = pl.multiple_of(chip * chip_rows, 8)
        value = pair_sum[piece, pl.ds(start, chip_rows)]
        for step in range(1, chips):
            chip_copy(piece, step).wait_recv()
            value = value + chip_in[piece * chips + step]
        chip_sum[piece] = value
        for step in range(1, cols):
            line_copy(piece, step).start()

    def line_stage(piece):
        start = pl.multiple_of(col * line_rows, 8)
        value = chip_sum[piece, pl.ds(start, line_rows)]
        for step in range(1, cols):
            line_copy(piece, step).wait_recv()
            value = value + line_in[piece * cols + step]
        line_sum[piece] = value
        line_out[piece, pl.ds(start, line_rows)] = value
        for step in range(1, cols):
            back_line_copy(piece, step).start()

    def back_line_stage(piece):
        for step in range(1, cols):
            back_line_copy(piece, step).wait_recv()
        start = pl.multiple_of(chip * chip_rows, 8)
        for step in range(1, chips):
            back_chip_copy(piece, step).start()
        chip_out[piece, pl.ds(start, chip_rows)] = line_out[piece]

    def back_chip_stage(piece):
        for step in range(1, chips):
            back_chip_copy(piece, step).wait_recv()
        back_pair_copy(piece).start()
        summed[piece, :, own_half()] = chip_out[piece]

    stages = (pair_stage, chip_stage, line_stage, back_line_stage, back_chip_stage)
    reached = [0] * pieces

    def advance(piece):
        if reached[piece] < len(stages):
            stages[reached[piece]](piece)
            reached[piece] += 1

    middle = rows // 2
    for mode in range(mode_count):
        lax.fori_loop(0, middle, back(mode), 0)
        for piece in range(mode):
            advance(piece)
        lax.fori_loop(middle, rows, back(mode), 0)
        for piece in range(mode - 1):
            advance(piece)
        pair_copy(mode).start()

    for index, (down, across) in enumerate(DIRECTIONS):

        @pl.when(inside(row + down, col + across, rows, cols))
        def _():
            object_halo(index).wait_send()

    accumulate()
    for index, (down, across) in enumerate(DIRECTIONS):
        if not down:
            start_halo(index)
    for piece in range(pieces):
        advance(piece)
    for index, (down, across) in enumerate(DIRECTIONS):
        if down:
            start_halo(index)
    folded[...] = gradient[:, half : half + tile, half : half + tile]
    for _ in stages:
        for piece in range(pieces):
            advance(piece)

    for index, (down, across) in enumerate(DIRECTIONS):

        @pl.when(inside(row - down, col - across, rows, cols))
        def _():
            halo(index).wait_recv()
            where = (slice(None), inner_edge(-down, tile, half), inner_edge(-across, tile, half))
            folded[where] += landing(index)[...]

    for piece in range(pieces):
        back_pair_copy(piece).wait_recv()
    for index, (down, across) in enumerate(DIRECTIONS):

        @pl.when(inside(row + down, col + across, rows, cols))
        def _():
            halo(index).wait_send()

    def sent(step, carry):
        slot_copy(step, row, lax.rem(row + step, rows)).wait_send()
        return carry

    lax.fori_loop(1, rows, sent, 0)
    for piece in range(pieces):
        pair_copy(piece).wait_send()
        back_pair_copy(piece).wait_send()
        for step in range(1, chips):
            chip_copy(piece, step).wait_send()
            back_chip_copy(piece, step).wait_send()
        for step in range(1, cols):
            line_copy(piece, step).wait_send()
            back_line_copy(piece, step).wait_send()


def whole(table, object_field, probe, raw_counts, delta, forward, backward):
    rows, cols = (lax.axis_size("row"), lax.axis_size("col"))
    tile = object_field.shape[1]
    modes, _, points, _ = probe.shape
    half = points // 2
    reach = tile + points
    length, lanes = (2 * points, points // 2)
    chips = rows // 2
    f32, bf16, i32 = (jnp.float32, jnp.bfloat16, jnp.int32)
    vmem = pl.BlockSpec(memory_space=pltpu.VMEM)
    hbm = pl.BlockSpec(memory_space=pl.ANY)
    dma = pltpu.SemaphoreType.DMA
    return pl.pallas_call(
        whole_kernel,
        name="whole",
        out_shape=(
            jax.ShapeDtypeStruct((2, tile, tile), f32),
            jax.ShapeDtypeStruct((modes, length, points), f32),
        ),
        in_specs=[pl.BlockSpec(memory_space=pltpu.SMEM)] + [hbm] * 6,
        out_specs=(vmem, vmem),
        scratch_shapes=[
            pltpu.VMEM(probe.shape, f32),
            pltpu.VMEM(raw_counts.shape, bf16),
            pltpu.VMEM(delta.shape, f32),
            pltpu.VMEM(forward.shape, bf16),
            pltpu.VMEM(backward.shape, bf16),
            pltpu.VMEM((2, reach, reach), f32),
            pltpu.VMEM((rows, points, points), bf16),
            pltpu.VMEM((rows, points, points), bf16),
            pltpu.VMEM((rows, 8, 128), i32),
            pltpu.VMEM((rows, 8, 128), i32),
            pltpu.SMEM((rows, 8, 128), i32),
            pltpu.VMEM((rows, 2, points, points), f32),
            pltpu.VMEM((rows, modes, points, 2 * points), bf16),
            pltpu.VMEM((modes, points, 2 * points), f32),
            pltpu.VMEM((rows, 2, points, points), f32),
            pltpu.VMEM((modes, length, points), f32),
            pltpu.VMEM((2 * tile + points, reach), f32),
            pltpu.VMEM((2, 2, tile, half), f32),
            pltpu.VMEM((2, 2, half, tile), f32),
            pltpu.VMEM((4, 2, half, half), f32),
            pltpu.VMEM((modes, length, lanes), f32),
            pltpu.VMEM((modes, length, lanes), f32),
            pltpu.VMEM((modes * chips, length // chips, lanes), f32),
            pltpu.VMEM((modes, length // chips, lanes), f32),
            pltpu.VMEM((modes * cols, length // chips // cols, lanes), f32),
            pltpu.VMEM((modes, length // chips // cols, lanes), f32),
            pltpu.VMEM((modes, length // chips, lanes), f32),
            pltpu.VMEM((modes, length, lanes), f32),
            dma((7,)),
            dma((8,)),
            dma((8,)),
            dma((rows,)),
            dma((rows,)),
            dma((rows,)),
            dma((rows,)),
            dma((8,)),
            dma((8,)),
            dma((2, modes)),
            dma((2, modes * chips)),
            dma((2, modes * cols)),
            dma((2, modes * cols)),
            dma((2, modes * chips)),
            dma((2, modes)),
        ],
        compiler_params=pltpu.CompilerParams(
            collective_id=0, has_side_effects=True, vmem_limit_bytes=67043328
        ),
    )(table, object_field, probe, raw_counts, delta, forward, backward)


def shards(object_field, probe, raw_counts, resample_delta, tile_row, offsets):
    points = probe.shape[-1]
    frame_total = raw_counts.shape[0] * lax.axis_size("row") * lax.axis_size("col")
    forward, backward = dft_tables(points)
    table = jnp.concatenate([tile_row, offsets], 1)
    object_grad, summed = whole(
        table, object_field, probe, raw_counts, resample_delta, forward, backward
    )
    return (object_grad, summed.reshape(probe.shape) * (1.0 / math.sqrt(frame_total)))


def solution(mesh):
    placed = (
        P(None, "row", "col"),
        P(),
        P(("row", "col"), None, None),
        P(),
        P(("row", "col"), None),
        P(("row", "col"), None),
    )
    return jax.shard_map(
        shards, mesh=mesh, in_specs=placed, out_specs=(P(None, "row", "col"), P()), check_vma=False
    )
```

```python
import math

import jax
import jax.numpy as jnp
import numpy as np
from jax import lax
from jax.experimental import pallas as pl
from jax.experimental.pallas import tpu as pltpu
from jax.sharding import PartitionSpec as P


MESH = pl.DeviceIdType.MESH
GROUP = 2
DIRECTIONS = tuple(
    (down, across) for down in (-1, 0, 1) for across in (-1, 0, 1) if (down, across) != (0, 0)
)


def place():
    return (
        lax.axis_index("row"),
        lax.axis_index("col"),
        lax.axis_size("row"),
        lax.axis_size("col"),
    )


def inside(row, col, rows, cols):
    return (row >= 0) & (row < rows) & (col >= 0) & (col < cols)


def inner_edge(step, tile, half):
    start, size = {-1: (0, half), 0: (0, tile), 1: (tile - half, half)}[step]
    return pl.ds(start, size)


def outer_edge(step, tile, half):
    start, size = {-1: (0, half), 0: (half, tile), 1: (half + tile, half)}[step]
    return pl.ds(start, size)


def greet():
    row, col, rows, cols = place()
    barrier = pltpu.get_barrier_semaphore()
    others = [(lax.rem(row + i, rows), col) for i in range(1, rows)]
    others += [(row, lax.rem(col + i, cols)) for i in range(1, cols)]
    for down in (1, rows - 1):
        for across in (1, cols - 1):
            others.append((lax.rem(row + down, rows), lax.rem(col + across, cols)))
    for other in others:
        pl.semaphore_signal(barrier, inc=1, device_id=other, device_id_type=MESH)
    pl.semaphore_wait(barrier, len(others))


def product(left, right):
    return jnp.dot(left, right, preferred_element_type=jnp.float32)


def dft_tables(points):
    indices = np.arange(points)
    angles = (indices[:, None] * indices[None, :] % points) * (2.0 * math.pi / points)
    cosine = np.cos(angles) / math.sqrt(points)
    sine_part = -np.sin(angles) / math.sqrt(points)
    forward = np.block([[cosine, -sine_part], [sine_part, cosine]])
    backward = np.block([[cosine, sine_part], [-sine_part, cosine]])
    return (jnp.asarray(forward, jnp.bfloat16), jnp.asarray(backward, jnp.bfloat16))


def whole_kernel(
    table,
    object_hbm,
    probe_hbm,
    raw_hbm,
    delta_hbm,
    forward_hbm,
    backward_hbm,
    folded,
    summed,
    probe,
    raw,
    delta,
    forward,
    backward,
    extended,
    incoming,
    outbox,
    infos,
    info_out,
    places,
    windows,
    residuals,
    far_field,
    terms,
    total,
    shifted,
    halos_tall,
    halos_wide,
    corners,
    pair_in,
    pair_sum,
    chip_in,
    chip_sum,
    line_in,
    line_sum,
    line_out,
    chip_out,
    local_sems,
    object_send,
    object_recv,
    slot_send,
    slot_recv,
    info_send,
    info_recv,
    halo_send,
    halo_recv,
    pair_sems,
    chip_sems,
    line_sems,
    back_line_sems,
    back_chip_sems,
    back_pair_sems,
):
    row, col, rows, cols = place()
    tile = folded.shape[1]
    points = raw.shape[1]
    half = points // 2
    reach = tile + points
    mode_count = probe.shape[0]
    frame_count = raw.shape[0]
    gradient = extended

    loads = [
        pltpu.make_async_copy(source, target, local_sems.at[i])
        for i, (source, target) in enumerate(
            (
                (raw_hbm, raw),
                (delta_hbm, delta),
                (object_hbm, extended.at[:, pl.ds(half, tile), pl.ds(half, tile)]),
                (probe_hbm, probe),
                (forward_hbm, forward),
                (backward_hbm, backward),
            )
        )
    ]
    for load in loads:
        load.start()
    greet()

    lanes_of = lax.broadcasted_iota(jnp.int32, (8, 128), 1)

    def chosen(other):
        pick, top, left, live = (jnp.int32(0), jnp.int32(0), jnp.int32(0), jnp.int32(0))
        for k in range(frame_count):
            hit = table[k, 0] == other
            pick = jnp.where(hit, k, pick)
            top = jnp.where(hit, table[k, 1], top)
            left = jnp.where(hit, table[k, 2], left)
            live = jnp.where(hit, 1, live)
        return pick, top, left, live

    def info_copy(step, target, other):
        return pltpu.make_async_remote_copy(
            src_ref=info_out.at[step],
            dst_ref=infos.at[target],
            send_sem=info_send.at[step],
            recv_sem=info_recv.at[target],
            device_id=(other, col),
            device_id_type=MESH,
        )

    def slot_copy(step, target, other):
        return pltpu.make_async_remote_copy(
            src_ref=outbox.at[step],
            dst_ref=incoming.at[target],
            send_sem=slot_send.at[step],
            recv_sem=slot_recv.at[target],
            device_id=(other, col),
            device_id_type=MESH,
        )

    def tell(step, carry):
        other = lax.rem(row + step, rows)
        _, top, left, live = chosen(other)
        info = jnp.where(lanes_of == 0, top, jnp.where(lanes_of == 1, left, live))

        @pl.when(step == 0)
        def _():
            infos[row] = info

        @pl.when(step > 0)
        def _():
            info_out[step] = info
            info_copy(step, row, other).start()

        return carry

    lax.fori_loop(0, rows, tell, 0)

    def object_halo(index):
        down, across = DIRECTIONS[index]
        return pltpu.make_async_remote_copy(
            src_ref=object_hbm.at[
                :, inner_edge(down, tile, half), inner_edge(across, tile, half)
            ],
            dst_ref=extended.at[
                :, outer_edge(-down, tile, half), outer_edge(-across, tile, half)
            ],
            send_sem=object_send.at[index],
            recv_sem=object_recv.at[index],
            device_id=(row + down, col + across),
            device_id_type=MESH,
        )

    for index, (down, across) in enumerate(DIRECTIONS):

        @pl.when(inside(row + down, col + across, rows, cols))
        def _():
            object_halo(index).start()

        @pl.when(jnp.logical_not(inside(row - down, col - across, rows, cols)))
        def _():
            where = (slice(None), outer_edge(-down, tile, half), outer_edge(-across, tile, half))
            extended[where] = jnp.zeros((2, where[1].size, where[2].size), jnp.float32)

    loads[0].wait()
    loads[1].wait()
    identity = (
        lax.broadcasted_iota(jnp.int32, (points, points), 0)
        == lax.broadcasted_iota(jnp.int32, (points, points), 1)
    ).astype(jnp.float32)
    resample = (identity + delta[...]).astype(jnp.bfloat16)

    def measure(step, carry):
        other = lax.rem(row + step, rows)
        pick, _, _, _ = chosen(other)
        first = product(resample, raw[pick]).astype(jnp.bfloat16)
        second = lax.dot_general(
            first, resample, (((1,), (1,)), ((), ())), preferred_element_type=jnp.float32
        )
        amplitude = jnp.sqrt(jnp.maximum(second, 0.0)).astype(jnp.bfloat16)

        @pl.when(step == 0)
        def _():
            incoming[row] = amplitude

        @pl.when(step > 0)
        def _():
            outbox[step] = amplitude
            slot_copy(step, row, other).start()

        return carry

    lax.fori_loop(0, rows, measure, 0)

    def heard(step, carry):
        source = lax.rem(row - step + rows, rows)
        info_copy(step, source, source).wait()
        return carry

    lax.fori_loop(1, rows, heard, 0)
    noted = pltpu.make_async_copy(infos, places, local_sems.at[6])
    noted.start()
    total[...] = jnp.zeros_like(total)
    shifted[...] = jnp.zeros_like(shifted)
    for load in loads[2:]:
        load.wait()
    noted.wait()
    for index, (down, across) in enumerate(DIRECTIONS):

        @pl.when(inside(row - down, col - across, rows, cols))
        def _():
            object_halo(index).wait_recv()

    span_rows, span_cols = (points + 8, points + 128)

    def spot(step):
        source = lax.rem(row - step + rows, rows)
        return source, places[source, 0, 0], places[source, 0, 1], places[source, 0, 2]

    def onward(step, carry):
        source, top, left, live = spot(step)
        skip_rows, skip_cols = (lax.rem(top, 8), lax.rem(left, 128))
        across_rows = pl.ds(lax.div(top, 8) * 8, span_rows)
        across_cols = pl.ds(lax.div(left, 128) * 128, span_cols)
        for part in range(2):
            block = extended[part, across_rows, across_cols]
            block = pltpu.roll(block, lax.rem(span_cols - skip_cols, span_cols), 1)
            block = block[:, :points]
            block = pltpu.roll(block, lax.rem(span_rows - skip_rows, span_rows), 0)
            windows[step, part] = block[:points]
        intensity = jnp.zeros((points, points), jnp.float32)
        halves = []
        for mode in range(mode_count):
            object_real, object_imag = (windows[step, 0], windows[step, 1])
            probe_real, probe_imag = (probe[mode, 0], probe[mode, 1])
            wave = jnp.concatenate(
                [
                    (probe_real * object_real - probe_imag * object_imag).astype(jnp.bfloat16),
                    (probe_real * object_imag + probe_imag * object_real).astype(jnp.bfloat16),
                ],
                0,
            )
            halves.append(product(forward[...], wave).astype(jnp.bfloat16))
        for mode, half_done in enumerate(halves):
            wave_rows = jnp.concatenate([half_done[:points], half_done[points:]], 1)
            field = product(wave_rows, backward[...])
            far_field[mode] = field
            squares = field * field
            intensity = intensity + squares[:, :points] + squares[:, points:]

        @pl.when(step > 0)
        def _():
            slot_copy(step, source, source).wait_recv()

        amplitude = incoming[source].astype(jnp.float32)
        scaling = 1.0 - amplitude / jnp.sqrt(jnp.maximum(intensity, 1.0))
        scaling = scaling * live.astype(jnp.float32)
        scaling = jnp.concatenate([scaling, scaling], 1)
        for mode in range(mode_count):
            residuals[step, mode] = (far_field[mode] * scaling).astype(jnp.bfloat16)
        return carry

    lax.fori_loop(0, rows, onward, 0)

    def back(mode, group):
        def one(index, carry):
            steps = [index * group + k for k in range(group)]
            backs = [
                product(residuals[step, mode], forward[...]).astype(jnp.bfloat16)
                for step in steps
            ]
            updates = [
                product(
                    backward[...], jnp.concatenate([rows_[:, :points], rows_[:, points:]], 0)
                )
                for rows_ in backs
            ]
            sum_real = total[mode, :points]
            sum_imag = total[mode, points:]
            for step, update in zip(steps, updates):
                update_real, update_imag = (update[:points], update[points:])
                object_real, object_imag = (windows[step, 0], windows[step, 1])
                probe_real, probe_imag = (probe[mode, 0], probe[mode, 1])
                term_real = probe_real * update_real + probe_imag * update_imag
                term_imag = probe_real * update_imag - probe_imag * update_real
                if mode == 0:
                    terms[step, 0] = term_real
                    terms[step, 1] = term_imag
                else:
                    terms[step, 0] += term_real
                    terms[step, 1] += term_imag
                sum_real = sum_real + (object_real * update_real + object_imag * update_imag)
                sum_imag = sum_imag + (object_real * update_imag - object_imag * update_real)
            total[mode, :points] = sum_real
            total[mode, points:] = sum_imag
            return carry

        return one

    def accumulate(begin, end):
        chunk = 64

        def one(step, carry):
            _, top, left, _ = spot(step)
            skip_rows, skip_cols = (lax.rem(top, 8), lax.rem(left, 128))
            base = tile // 8 - lax.div(top, 8)
            across = (tile // 128 - 1 - lax.div(left, 128)) * 128
            for part in range(2):
                block = jnp.concatenate(
                    [terms[step, part], jnp.zeros((8, points), jnp.float32)], 0
                )
                block = pltpu.roll(block, skip_rows, 0)
                block = jnp.concatenate([block, jnp.zeros((span_rows, 128), jnp.float32)], 1)
                shifted[pl.ds(tile, span_rows), pl.ds(tile - 128, span_cols)] = pltpu.roll(
                    block, skip_cols, 1
                )

                def add(index, inner):
                    start = pl.multiple_of(index * chunk, 8)
                    source = (base + index * (chunk // 8)) * 8
                    gradient[part, pl.ds(start, chunk)] += shifted[
                        pl.ds(source, chunk), pl.ds(across, reach)
                    ]
                    return inner

                lax.fori_loop(0, reach // chunk, add, 0)
            return carry

        lax.fori_loop(begin, end, one, 0)

    pieces = pair_in.shape[0]
    length = pair_in.shape[1]
    chips = rows // 2
    core, chip = (lax.rem(row, 2), row // 2)
    chip_rows = length // chips
    line_rows = chip_rows // cols
    lanes = summed.shape[2] // 2

    def own_half():
        return pl.ds(pl.multiple_of(core * lanes, lanes), lanes)

    def sibling_half():
        return pl.ds(pl.multiple_of((1 - core) * lanes, lanes), lanes)

    sibling = (row + 1 - 2 * core, col)
    def landing(index):
        down, across = DIRECTIONS[index]
        if down and across:
            return corners.at[(down + 1) + (across + 1) // 2]
        return halos_wide.at[(down + 1) // 2] if down else halos_tall.at[(across + 1) // 2]

    def halo(index):
        down, across = DIRECTIONS[index]
        return pltpu.make_async_remote_copy(
            src_ref=gradient.at[:, outer_edge(down, tile, half), outer_edge(across, tile, half)],
            dst_ref=landing(index),
            send_sem=halo_send.at[index],
            recv_sem=halo_recv.at[index],
            device_id=(row + down, col + across),
            device_id_type=MESH,
        )

    def start_halo(index):
        down, across = DIRECTIONS[index]

        @pl.when(inside(row + down, col + across, rows, cols))
        def _():
            halo(index).start()

    def remote(source, target, sems, index, device):
        return pltpu.make_async_remote_copy(
            src_ref=source,
            dst_ref=target,
            send_sem=sems.at[0, index],
            recv_sem=sems.at[1, index],
            device_id=device,
            device_id_type=MESH,
        )

    def pair_copy(piece):
        return remote(
            total.at[piece, :, sibling_half()], pair_in.at[piece], pair_sems, piece, sibling
        )

    def chip_copy(piece, step):
        other = lax.rem(chip + step, chips)
        start = pl.multiple_of(other * chip_rows, 8)
        index = piece * chips + step
        return remote(
            pair_sum.at[piece, pl.ds(start, chip_rows)],
            chip_in.at[index],
            chip_sems,
            index,
            (2 * other + core, col),
        )

    def line_copy(piece, step):
        other = lax.rem(col + step, cols)
        start = pl.multiple_of(other * line_rows, 8)
        index = piece * cols + step
        return remote(
            chip_sum.at[piece, pl.ds(start, line_rows)],
            line_in.at[index],
            line_sems,
            index,
            (row, other),
        )

    def back_line_copy(piece, step):
        other = lax.rem(col + step, cols)
        start = pl.multiple_of(col * line_rows, 8)
        return remote(
            line_sum.at[piece],
            line_out.at[piece, pl.ds(start, line_rows)],
            back_line_sems,
            piece * cols + step,
            (row, other),
        )

    def back_chip_copy(piece, step):
        other = lax.rem(chip + step, chips)
        start = pl.multiple_of(chip * chip_rows, 8)
        return remote(
            line_out.at[piece],
            chip_out.at[piece, pl.ds(start, chip_rows)],
            back_chip_sems,
            piece * chips + step,
            (2 * other + core, col),
        )

    def back_pair_copy(piece):
        return remote(
            chip_out.at[piece],
            summed.at[piece, :, own_half()],
            back_pair_sems,
            piece,
            sibling,
        )

    def pair_stage(piece):
        pair_copy(piece).wait_recv()
        pair_sum[piece] = total[piece, :, own_half()] + pair_in[piece]
        for step in range(1, chips):
            chip_copy(piece, step).start()

    def chip_stage(piece):
        start = pl.multiple_of(chip * chip_rows, 8)
        value = pair_sum[piece, pl.ds(start, chip_rows)]
        for step in range(1, chips):
            chip_copy(piece, step).wait_recv()
            value = value + chip_in[piece * chips + step]
        chip_sum[piece] = value
        for step in range(1, cols):
            line_copy(piece, step).start()

    def line_stage(piece):
        start = pl.multiple_of(col * line_rows, 8)
        value = chip_sum[piece, pl.ds(start, line_rows)]
        for step in range(1, cols):
            line_copy(piece, step).wait_recv()
            value = value + line_in[piece * cols + step]
        line_sum[piece] = value
        line_out[piece, pl.ds(start, line_rows)] = value
        for step in range(1, cols):
            back_line_copy(piece, step).start()

    def back_line_stage(piece):
        for step in range(1, cols):
            back_line_copy(piece, step).wait_recv()
        start = pl.multiple_of(chip * chip_rows, 8)
        for step in range(1, chips):
            back_chip_copy(piece, step).start()
        chip_out[piece, pl.ds(start, chip_rows)] = line_out[piece]

    def back_chip_stage(piece):
        for step in range(1, chips):
            back_chip_copy(piece, step).wait_recv()
        back_pair_copy(piece).start()
        summed[piece, :, own_half()] = chip_out[piece]

    stages = (pair_stage, chip_stage, line_stage, back_line_stage, back_chip_stage)
    reached = [0] * pieces

    def advance(piece):
        if reached[piece] < len(stages):
            stages[reached[piece]](piece)
            reached[piece] += 1

    middle = rows // 2 // GROUP
    for mode in range(mode_count):
        lax.fori_loop(0, middle, back(mode, GROUP), 0)
        for piece in range(mode):
            advance(piece)
        lax.fori_loop(middle, 2 * middle, back(mode, GROUP), 0)
        for piece in range(mode - 1):
            advance(piece)
        pair_copy(mode).start()

    for index, (down, across) in enumerate(DIRECTIONS):

        @pl.when(inside(row + down, col + across, rows, cols))
        def _():
            object_halo(index).wait_send()

    gradient[...] = jnp.zeros_like(gradient)
    plan = ((1, 2), (0,), (1, 2), (0,))
    for quarter, which in enumerate(plan):
        accumulate(quarter * rows // 4, (quarter + 1) * rows // 4)
        for piece in which:
            advance(piece)
    for index, (down, across) in enumerate(DIRECTIONS):
        start_halo(index)
    folded[...] = gradient[:, half : half + tile, half : half + tile]
    for _ in stages:
        for piece in range(pieces):
            advance(piece)

    for index, (down, across) in enumerate(DIRECTIONS):

        @pl.when(inside(row - down, col - across, rows, cols))
        def _():
            halo(index).wait_recv()
            where = (slice(None), inner_edge(-down, tile, half), inner_edge(-across, tile, half))
            folded[where] += landing(index)[...]

    for piece in range(pieces):
        back_pair_copy(piece).wait_recv()
    for index, (down, across) in enumerate(DIRECTIONS):

        @pl.when(inside(row + down, col + across, rows, cols))
        def _():
            halo(index).wait_send()

    def sent(step, carry):
        slot_copy(step, row, lax.rem(row + step, rows)).wait_send()
        return carry

    lax.fori_loop(1, rows, sent, 0)
    for piece in range(pieces):
        pair_copy(piece).wait_send()
        back_pair_copy(piece).wait_send()
        for step in range(1, chips):
            chip_copy(piece, step).wait_send()
            back_chip_copy(piece, step).wait_send()
        for step in range(1, cols):
            line_copy(piece, step).wait_send()
            back_line_copy(piece, step).wait_send()


def whole(table, object_field, probe, raw_counts, delta, forward, backward):
    rows, cols = (lax.axis_size("row"), lax.axis_size("col"))
    tile = object_field.shape[1]
    modes, _, points, _ = probe.shape
    half = points // 2
    reach = tile + points
    length, lanes = (2 * points, points // 2)
    chips = rows // 2
    f32, bf16, i32 = (jnp.float32, jnp.bfloat16, jnp.int32)
    vmem = pl.BlockSpec(memory_space=pltpu.VMEM)
    hbm = pl.BlockSpec(memory_space=pl.ANY)
    dma = pltpu.SemaphoreType.DMA
    return pl.pallas_call(
        whole_kernel,
        name="whole",
        out_shape=(
            jax.ShapeDtypeStruct((2, tile, tile), f32),
            jax.ShapeDtypeStruct((modes, length, points), f32),
        ),
        in_specs=[pl.BlockSpec(memory_space=pltpu.SMEM)] + [hbm] * 6,
        out_specs=(vmem, vmem),
        scratch_shapes=[
            pltpu.VMEM(probe.shape, f32),
            pltpu.VMEM(raw_counts.shape, bf16),
            pltpu.VMEM(delta.shape, f32),
            pltpu.VMEM(forward.shape, bf16),
            pltpu.VMEM(backward.shape, bf16),
            pltpu.VMEM((2, reach, reach), f32),
            pltpu.VMEM((rows, points, points), bf16),
            pltpu.VMEM((rows, points, points), bf16),
            pltpu.VMEM((rows, 8, 128), i32),
            pltpu.VMEM((rows, 8, 128), i32),
            pltpu.SMEM((rows, 8, 128), i32),
            pltpu.VMEM((rows, 2, points, points), f32),
            pltpu.VMEM((rows, modes, points, 2 * points), bf16),
            pltpu.VMEM((modes, points, 2 * points), f32),
            pltpu.VMEM((rows, 2, points, points), f32),
            pltpu.VMEM((modes, length, points), f32),
            pltpu.VMEM((2 * tile + points, 2 * tile + half), f32),
            pltpu.VMEM((2, 2, tile, half), f32),
            pltpu.VMEM((2, 2, half, tile), f32),
            pltpu.VMEM((4, 2, half, half), f32),
            pltpu.VMEM((modes, length, lanes), f32),
            pltpu.VMEM((modes, length, lanes), f32),
            pltpu.VMEM((modes * chips, length // chips, lanes), f32),
            pltpu.VMEM((modes, length // chips, lanes), f32),
            pltpu.VMEM((modes * cols, length // chips // cols, lanes), f32),
            pltpu.VMEM((modes, length // chips // cols, lanes), f32),
            pltpu.VMEM((modes, length // chips, lanes), f32),
            pltpu.VMEM((modes, length, lanes), f32),
            dma((7,)),
            dma((8,)),
            dma((8,)),
            dma((rows,)),
            dma((rows,)),
            dma((rows,)),
            dma((rows,)),
            dma((8,)),
            dma((8,)),
            dma((2, modes)),
            dma((2, modes * chips)),
            dma((2, modes * cols)),
            dma((2, modes * cols)),
            dma((2, modes * chips)),
            dma((2, modes)),
        ],
        compiler_params=pltpu.CompilerParams(
            collective_id=0, has_side_effects=True, vmem_limit_bytes=67043328
        ),
    )(table, object_field, probe, raw_counts, delta, forward, backward)


def shards(object_field, probe, raw_counts, resample_delta, tile_row, offsets):
    points = probe.shape[-1]
    frame_total = raw_counts.shape[0] * lax.axis_size("row") * lax.axis_size("col")
    forward, backward = dft_tables(points)
    table = jnp.concatenate([tile_row, offsets], 1)
    object_grad, summed = whole(
        table, object_field, probe, raw_counts, resample_delta, forward, backward
    )
    return (object_grad, summed.reshape(probe.shape) * (1.0 / math.sqrt(frame_total)))


def solution(mesh):
    placed = (
        P(None, "row", "col"),
        P(),
        P(("row", "col"), None, None),
        P(),
        P(("row", "col"), None),
        P(("row", "col"), None),
    )
    return jax.shard_map(
        shards, mesh=mesh, in_specs=placed, out_specs=(P(None, "row", "col"), P()), check_vma=False
    )
```

```python
import math

import jax
import jax.numpy as jnp
import numpy as np
from jax import lax
from jax.experimental import pallas as pl
from jax.experimental.pallas import tpu as pltpu
from jax.sharding import PartitionSpec as P


MESH = pl.DeviceIdType.MESH
GROUP = 2
WAYS = 4
DIRECTIONS = tuple(
    (down, across) for down in (-1, 0, 1) for across in (-1, 0, 1) if (down, across) != (0, 0)
)


def place():
    return (
        lax.axis_index("row"),
        lax.axis_index("col"),
        lax.axis_size("row"),
        lax.axis_size("col"),
    )


def inside(row, col, rows, cols):
    return (row >= 0) & (row < rows) & (col >= 0) & (col < cols)


def inner_edge(step, tile, half):
    start, size = {-1: (0, half), 0: (0, tile), 1: (tile - half, half)}[step]
    return pl.ds(start, size)


def outer_edge(step, tile, half):
    start, size = {-1: (0, half), 0: (half, tile), 1: (half + tile, half)}[step]
    return pl.ds(start, size)


LEVELS = 32767.0


def coded(value, bound):
    level = jnp.sqrt(jnp.abs(value) * (1.0 / bound)) * LEVELS
    level = jnp.where(value < 0.0, -level, level)
    return jnp.round(level).astype(jnp.int32).astype(jnp.int16)


def decoded(code, bound):
    level = code.astype(jnp.int32).astype(jnp.float32) * (1.0 / LEVELS)
    return level * jnp.abs(level) * bound


def greatest(value):
    return jnp.maximum(jnp.max(jnp.abs(value)), 1e-30)


def greet():
    row, col, rows, cols = place()
    barrier = pltpu.get_barrier_semaphore()
    others = [(lax.rem(row + i, rows), col) for i in range(1, rows)]
    others += [(row, lax.rem(col + i, cols)) for i in range(1, cols)]
    for down in (1, rows - 1):
        for across in (1, cols - 1):
            others.append((lax.rem(row + down, rows), lax.rem(col + across, cols)))
    for other in others:
        pl.semaphore_signal(barrier, inc=1, device_id=other, device_id_type=MESH)
    pl.semaphore_wait(barrier, len(others))


def product(left, right):
    return jnp.dot(left, right, preferred_element_type=jnp.float32)


def dft_tables(points):
    indices = np.arange(points)
    angles = (indices[:, None] * indices[None, :] % points) * (2.0 * math.pi / points)
    cosine = np.cos(angles) / math.sqrt(points)
    sine_part = -np.sin(angles) / math.sqrt(points)
    forward = np.block([[cosine, -sine_part], [sine_part, cosine]])
    backward = np.block([[cosine, sine_part], [-sine_part, cosine]])
    return (jnp.asarray(forward, jnp.bfloat16), jnp.asarray(backward, jnp.bfloat16))


def whole_kernel(
    tile_row,
    offsets,
    object_hbm,
    probe_hbm,
    raw_hbm,
    delta_hbm,
    forward_hbm,
    backward_hbm,
    folded,
    summed,
    probe,
    raw,
    delta,
    forward,
    backward,
    extended,
    incoming,
    outbox,
    infos,
    info_out,
    places,
    windows,
    residuals,
    far_field,
    terms,
    total,
    shifted,
    code_tall,
    code_wide,
    code_corners,
    halos_tall,
    halos_wide,
    corners,
    bound_out,
    bounds,
    pair_in,
    pair_sum,
    chip_in,
    chip_sum,
    line_in,
    line_sum,
    line_out,
    chip_out,
    local_sems,
    object_send,
    object_recv,
    slot_send,
    slot_recv,
    info_send,
    info_recv,
    halo_send,
    halo_recv,
    bound_send,
    bound_recv,
    pair_sems,
    chip_sems,
    line_sems,
    back_line_sems,
    back_chip_sems,
    back_pair_sems,
):
    row, col, rows, cols = place()
    tile = folded.shape[1]
    points = raw.shape[1]
    half = points // 2
    reach = tile + points
    mode_count = probe.shape[0]
    frame_count = raw.shape[0]
    gradient = extended

    loads = [
        pltpu.make_async_copy(source, target, local_sems.at[i])
        for i, (source, target) in enumerate(
            (
                (raw_hbm, raw),
                (delta_hbm, delta),
                (object_hbm, extended.at[:, pl.ds(half, tile), pl.ds(half, tile)]),
                (probe_hbm, probe),
                (forward_hbm, forward),
                (backward_hbm, backward),
            )
        )
    ]
    for load in loads:
        load.start()
    greet()

    lanes_of = lax.broadcasted_iota(jnp.int32, (8, 128), 1)

    def chosen(other):
        pick, top, left, live = (jnp.int32(0), jnp.int32(0), jnp.int32(0), jnp.int32(0))
        for k in range(frame_count):
            hit = tile_row[k, 0] == other
            pick = jnp.where(hit, k, pick)
            top = jnp.where(hit, offsets[k, 0], top)
            left = jnp.where(hit, offsets[k, 1], left)
            live = jnp.where(hit, 1, live)
        return pick, top, left, live

    def info_copy(step, target, other):
        return pltpu.make_async_remote_copy(
            src_ref=info_out.at[step],
            dst_ref=infos.at[target],
            send_sem=info_send.at[step],
            recv_sem=info_recv.at[target],
            device_id=(other, col),
            device_id_type=MESH,
        )

    def slot_copy(step, target, other):
        return pltpu.make_async_remote_copy(
            src_ref=outbox.at[step],
            dst_ref=incoming.at[target],
            send_sem=slot_send.at[step],
            recv_sem=slot_recv.at[target],
            device_id=(other, col),
            device_id_type=MESH,
        )

    def tell(step, carry):
        other = lax.rem(row + step, rows)
        _, top, left, live = chosen(other)
        info = jnp.where(lanes_of == 0, top, jnp.where(lanes_of == 1, left, live))

        @pl.when(step == 0)
        def _():
            infos[row] = info

        @pl.when(step > 0)
        def _():
            info_out[step] = info
            info_copy(step, row, other).start()

        return carry

    lax.fori_loop(0, rows, tell, 0)

    def pick(tall, wide, corner, index, part):
        down, across = DIRECTIONS[index]
        if down and across:
            return corner.at[(down + 1) + (across + 1) // 2, part]
        return wide.at[(down + 1) // 2, part] if down else tall.at[(across + 1) // 2, part]

    def bound_copy(index):
        down, across = DIRECTIONS[index]
        return pltpu.make_async_remote_copy(
            src_ref=bound_out,
            dst_ref=bounds.at[index],
            send_sem=bound_send.at[index],
            recv_sem=bound_recv.at[index],
            device_id=(row + down, col + across),
            device_id_type=MESH,
        )

    def object_halo(index):
        down, across = DIRECTIONS[index]
        return pltpu.make_async_remote_copy(
            src_ref=object_hbm.at[
                :, inner_edge(down, tile, half), inner_edge(across, tile, half)
            ],
            dst_ref=extended.at[
                :, outer_edge(-down, tile, half), outer_edge(-across, tile, half)
            ],
            send_sem=object_send.at[index],
            recv_sem=object_recv.at[index],
            device_id=(row + down, col + across),
            device_id_type=MESH,
        )

    for index, (down, across) in enumerate(DIRECTIONS):

        @pl.when(inside(row + down, col + across, rows, cols))
        def _():
            object_halo(index).start()

        @pl.when(jnp.logical_not(inside(row - down, col - across, rows, cols)))
        def _():
            where = (slice(None), outer_edge(-down, tile, half), outer_edge(-across, tile, half))
            extended[where] = jnp.zeros((2, where[1].size, where[2].size), jnp.float32)

    loads[0].wait()
    loads[1].wait()
    identity = (
        lax.broadcasted_iota(jnp.int32, (points, points), 0)
        == lax.broadcasted_iota(jnp.int32, (points, points), 1)
    ).astype(jnp.float32)
    resample = (identity + delta[...]).astype(jnp.bfloat16)

    def measure(step, carry):
        other = lax.rem(row + step, rows)
        pick, _, _, _ = chosen(other)
        first = product(resample, raw[pick]).astype(jnp.bfloat16)
        second = lax.dot_general(
            first, resample, (((1,), (1,)), ((), ())), preferred_element_type=jnp.float32
        )
        amplitude = jnp.sqrt(jnp.maximum(second, 0.0)).astype(jnp.bfloat16)

        @pl.when(step == 0)
        def _():
            incoming[row] = amplitude

        @pl.when(step > 0)
        def _():
            outbox[step] = amplitude
            slot_copy(step, row, other).start()

        return carry

    lax.fori_loop(0, rows, measure, 0)

    def heard(step, carry):
        source = lax.rem(row - step + rows, rows)
        info_copy(step, source, source).wait()
        return carry

    lax.fori_loop(1, rows, heard, 0)
    noted = pltpu.make_async_copy(infos, places, local_sems.at[6])
    noted.start()
    total[...] = jnp.zeros_like(total)
    shifted[...] = jnp.zeros_like(shifted)
    for load in loads[2:]:
        load.wait()
    noted.wait()
    for index, (down, across) in enumerate(DIRECTIONS):

        @pl.when(inside(row - down, col - across, rows, cols))
        def _():
            object_halo(index).wait_recv()

    span_rows, span_cols = (points + 8, points + 128)

    def spot(step):
        source = lax.rem(row - step + rows, rows)
        return source, places[source, 0, 0], places[source, 0, 1], places[source, 0, 2]

    def onward(step, carry):
        source, top, left, live = spot(step)
        skip_rows, skip_cols = (lax.rem(top, 8), lax.rem(left, 128))
        across_rows = pl.ds(lax.div(top, 8) * 8, span_rows)
        across_cols = pl.ds(lax.div(left, 128) * 128, span_cols)
        for part in range(2):
            block = extended[part, across_rows, across_cols]
            block = pltpu.roll(block, lax.rem(span_cols - skip_cols, span_cols), 1)
            block = block[:, :points]
            block = pltpu.roll(block, lax.rem(span_rows - skip_rows, span_rows), 0)
            windows[step, part] = block[:points]
        intensity = jnp.zeros((points, points), jnp.float32)
        halves = []
        for mode in range(mode_count):
            object_real, object_imag = (windows[step, 0], windows[step, 1])
            probe_real, probe_imag = (probe[mode, 0], probe[mode, 1])
            wave = jnp.concatenate(
                [
                    (probe_real * object_real - probe_imag * object_imag).astype(jnp.bfloat16),
                    (probe_real * object_imag + probe_imag * object_real).astype(jnp.bfloat16),
                ],
                0,
            )
            halves.append(product(forward[...], wave).astype(jnp.bfloat16))
        for mode, half_done in enumerate(halves):
            wave_rows = jnp.concatenate([half_done[:points], half_done[points:]], 1)
            field = product(wave_rows, backward[...])
            far_field[mode] = field
            squares = field * field
            intensity = intensity + squares[:, :points] + squares[:, points:]

        @pl.when(step > 0)
        def _():
            slot_copy(step, source, source).wait_recv()

        amplitude = incoming[source].astype(jnp.float32)
        scaling = 1.0 - amplitude / jnp.sqrt(jnp.maximum(intensity, 1.0))
        scaling = scaling * live.astype(jnp.float32)
        scaling = jnp.concatenate([scaling, scaling], 1)
        for mode in range(mode_count):
            residuals[step, mode] = (far_field[mode] * scaling).astype(jnp.bfloat16)
        return carry

    lax.fori_loop(0, rows, onward, 0)

    def back(mode, group):
        def one(index, carry):
            steps = [index * group + k for k in range(group)]
            backs = [
                product(residuals[step, mode], forward[...]).astype(jnp.bfloat16)
                for step in steps
            ]
            updates = [
                product(
                    backward[...], jnp.concatenate([rows_[:, :points], rows_[:, points:]], 0)
                )
                for rows_ in backs
            ]
            sum_real = total[mode, :points]
            sum_imag = total[mode, points:]
            for step, update in zip(steps, updates):
                update_real, update_imag = (update[:points], update[points:])
                object_real, object_imag = (windows[step, 0], windows[step, 1])
                probe_real, probe_imag = (probe[mode, 0], probe[mode, 1])
                term_real = probe_real * update_real + probe_imag * update_imag
                term_imag = probe_real * update_imag - probe_imag * update_real
                if mode == 0:
                    terms[step, 0] = term_real
                    terms[step, 1] = term_imag
                else:
                    terms[step, 0] += term_real
                    terms[step, 1] += term_imag
                sum_real = sum_real + (object_real * update_real + object_imag * update_imag)
                sum_imag = sum_imag + (object_real * update_imag - object_imag * update_real)
            total[mode, :points] = sum_real
            total[mode, points:] = sum_imag
            return carry

        return one

    ways = shifted.shape[0]

    def accumulate(group):
        chunk = 32
        first = group * ways
        found = [spot(first + k) for k in range(ways)]
        bases = [tile // 8 - lax.div(top, 8) for _, top, _, _ in found]
        acrosses = [(tile // 128 - 1 - lax.div(left, 128)) * 128 for _, _, left, _ in found]
        for part in range(2):
            for k in range(ways):
                _, top, left, _ = found[k]
                block = jnp.concatenate(
                    [terms[first + k, part], jnp.zeros((8, points), jnp.float32)], 0
                )
                block = pltpu.roll(block, lax.rem(top, 8), 0)
                block = jnp.concatenate([block, jnp.zeros((span_rows, 128), jnp.float32)], 1)
                shifted[k, pl.ds(tile, span_rows), pl.ds(tile - 128, span_cols)] = pltpu.roll(
                    block, lax.rem(left, 128), 1
                )

            def add(index, inner):
                start = pl.multiple_of(index * chunk, 8)
                value = gradient[part, pl.ds(start, chunk)]
                for k in range(ways):
                    source = (bases[k] + index * (chunk // 8)) * 8
                    value = value + shifted[k, pl.ds(source, chunk), pl.ds(acrosses[k], reach)]
                gradient[part, pl.ds(start, chunk)] = value
                return inner

            lax.fori_loop(0, reach // chunk, add, 0)

    pieces = pair_in.shape[0]
    length = pair_in.shape[1]
    chips = rows // 2
    core, chip = (lax.rem(row, 2), row // 2)
    chip_rows = length // chips
    line_rows = chip_rows // cols
    lanes = summed.shape[2] // 2

    def own_half():
        return pl.ds(pl.multiple_of(core * lanes, lanes), lanes)

    def sibling_half():
        return pl.ds(pl.multiple_of((1 - core) * lanes, lanes), lanes)

    sibling = (row + 1 - 2 * core, col)
    def halo(index, part):
        down, across = DIRECTIONS[index]
        return pltpu.make_async_remote_copy(
            src_ref=pick(code_tall, code_wide, code_corners, index, part),
            dst_ref=pick(halos_tall, halos_wide, corners, index, part),
            send_sem=halo_send.at[part, index],
            recv_sem=halo_recv.at[part, index],
            device_id=(row + down, col + across),
            device_id_type=MESH,
        )

    def encode(part, bound):
        for index, (down, across) in enumerate(DIRECTIONS):
            where = (part, outer_edge(down, tile, half), outer_edge(across, tile, half))
            pick(code_tall, code_wide, code_corners, index, part)[...] = coded(
                gradient[where], bound
            )

    def start_halos(part):
        for index, (down, across) in enumerate(DIRECTIONS):

            @pl.when(inside(row + down, col + across, rows, cols))
            def _():
                if part == 0:
                    bound_copy(index).start()
                halo(index, part).start()

    def take_halos(part):
        for index, (down, across) in enumerate(DIRECTIONS):

            @pl.when(inside(row - down, col - across, rows, cols))
            def _():
                if part == 0:
                    bound_copy(index).wait_recv()
                halo(index, part).wait_recv()
                where = (part, inner_edge(-down, tile, half), inner_edge(-across, tile, half))
                folded[where] += decoded(
                    pick(halos_tall, halos_wide, corners, index, part)[...],
                    jnp.max(bounds[index]),
                )

    def remote(source, target, sems, index, device):
        return pltpu.make_async_remote_copy(
            src_ref=source,
            dst_ref=target,
            send_sem=sems.at[0, index],
            recv_sem=sems.at[1, index],
            device_id=device,
            device_id_type=MESH,
        )

    def pair_copy(piece):
        return remote(
            total.at[piece, :, sibling_half()], pair_in.at[piece], pair_sems, piece, sibling
        )

    def chip_copy(piece, step):
        other = lax.rem(chip + step, chips)
        start = pl.multiple_of(other * chip_rows, 8)
        index = piece * chips + step
        return remote(
            pair_sum.at[piece, pl.ds(start, chip_rows)],
            chip_in.at[index],
            chip_sems,
            index,
            (2 * other + core, col),
        )

    def line_copy(piece, step):
        other = lax.rem(col + step, cols)
        start = pl.multiple_of(other * line_rows, 8)
        index = piece * cols + step
        return remote(
            chip_sum.at[piece, pl.ds(start, line_rows)],
            line_in.at[index],
            line_sems,
            index,
            (row, other),
        )

    def back_line_copy(piece, step):
        other = lax.rem(col + step, cols)
        start = pl.multiple_of(col * line_rows, 8)
        return remote(
            line_sum.at[piece],
            line_out.at[piece, pl.ds(start, line_rows)],
            back_line_sems,
            piece * cols + step,
            (row, other),
        )

    def back_chip_copy(piece, step):
        other = lax.rem(chip + step, chips)
        start = pl.multiple_of(chip * chip_rows, 8)
        return remote(
            line_out.at[piece],
            chip_out.at[piece, pl.ds(start, chip_rows)],
            back_chip_sems,
            piece * chips + step,
            (2 * other + core, col),
        )

    def back_pair_copy(piece):
        return remote(
            chip_out.at[piece],
            summed.at[piece, :, own_half()],
            back_pair_sems,
            piece,
            sibling,
        )

    def pair_stage(piece):
        pair_copy(piece).wait_recv()
        pair_sum[piece] = total[piece, :, own_half()] + pair_in[piece]
        for step in range(1, chips):
            chip_copy(piece, step).start()

    def chip_stage(piece):
        start = pl.multiple_of(chip * chip_rows, 8)
        value = pair_sum[piece, pl.ds(start, chip_rows)]
        for step in range(1, chips):
            chip_copy(piece, step).wait_recv()
            value = value + chip_in[piece * chips + step]
        chip_sum[piece] = value
        for step in range(1, cols):
            line_copy(piece, step).start()

    def line_stage(piece):
        start = pl.multiple_of(col * line_rows, 8)
        value = chip_sum[piece, pl.ds(start, line_rows)]
        for step in range(1, cols):
            line_copy(piece, step).wait_recv()
            value = value + line_in[piece * cols + step]
        line_sum[piece] = value
        line_out[piece, pl.ds(start, line_rows)] = value
        for step in range(1, cols):
            back_line_copy(piece, step).start()

    def back_line_stage(piece):
        for step in range(1, cols):
            back_line_copy(piece, step).wait_recv()
        start = pl.multiple_of(chip * chip_rows, 8)
        for step in range(1, chips):
            back_chip_copy(piece, step).start()
        chip_out[piece, pl.ds(start, chip_rows)] = line_out[piece]

    def back_chip_stage(piece):
        for step in range(1, chips):
            back_chip_copy(piece, step).wait_recv()
        back_pair_copy(piece).start()
        summed[piece, :, own_half()] = chip_out[piece]

    stages = (pair_stage, chip_stage, line_stage, back_line_stage, back_chip_stage)
    reached = [0] * pieces

    def advance(piece):
        if reached[piece] < len(stages):
            stages[reached[piece]](piece)
            reached[piece] += 1

    middle = rows // 2 // GROUP
    for mode in range(mode_count):
        lax.fori_loop(0, middle, back(mode, GROUP), 0)
        for piece in range(mode):
            advance(piece)
        lax.fori_loop(middle, 2 * middle, back(mode, GROUP), 0)
        for piece in range(mode - 1):
            advance(piece)
        pair_copy(mode).start()

    for index, (down, across) in enumerate(DIRECTIONS):

        @pl.when(inside(row + down, col + across, rows, cols))
        def _():
            object_halo(index).wait_send()

    gradient[...] = jnp.zeros_like(gradient)
    passes = rows // ways
    plan = (1, 2, 0, 1, 2, 0)
    done = 0
    for group in range(passes):
        accumulate(group)
        until = len(plan) * (group + 1) // passes
        for piece in plan[done:until]:
            advance(piece)
        done = until
    bound = greatest(gradient[...])
    bound_out[...] = jnp.full((8, 128), bound, jnp.float32)
    encode(0, bound)
    advance(1)
    start_halos(0)
    encode(1, bound)
    advance(2)
    folded[...] = gradient[:, half : half + tile, half : half + tile]
    advance(2)
    start_halos(1)
    for _ in stages:
        for piece in range(pieces):
            advance(piece)
    take_halos(0)
    take_halos(1)
    for piece in range(pieces):
        back_pair_copy(piece).wait_recv()
    for index, (down, across) in enumerate(DIRECTIONS):

        @pl.when(inside(row + down, col + across, rows, cols))
        def _():
            bound_copy(index).wait_send()
            halo(index, 0).wait_send()
            halo(index, 1).wait_send()

    def sent(step, carry):
        slot_copy(step, row, lax.rem(row + step, rows)).wait_send()
        return carry

    lax.fori_loop(1, rows, sent, 0)
    for piece in range(pieces):
        pair_copy(piece).wait_send()
        back_pair_copy(piece).wait_send()
        for step in range(1, chips):
            chip_copy(piece, step).wait_send()
            back_chip_copy(piece, step).wait_send()
        for step in range(1, cols):
            line_copy(piece, step).wait_send()
            back_line_copy(piece, step).wait_send()


def whole(tile_row, offsets, object_field, probe, raw_counts, delta, forward, backward):
    rows, cols = (lax.axis_size("row"), lax.axis_size("col"))
    tile = object_field.shape[1]
    modes, _, points, _ = probe.shape
    half = points // 2
    reach = tile + points
    length, lanes = (2 * points, points // 2)
    chips = rows // 2
    f32, bf16, i32, i16 = (jnp.float32, jnp.bfloat16, jnp.int32, jnp.int16)
    vmem = pl.BlockSpec(memory_space=pltpu.VMEM)
    hbm = pl.BlockSpec(memory_space=pl.ANY)
    dma = pltpu.SemaphoreType.DMA
    return pl.pallas_call(
        whole_kernel,
        name="whole",
        out_shape=(
            jax.ShapeDtypeStruct((2, tile, tile), f32),
            jax.ShapeDtypeStruct((modes, length, points), f32),
        ),
        in_specs=[pl.BlockSpec(memory_space=pltpu.SMEM)] * 2 + [hbm] * 6,
        out_specs=(vmem, vmem),
        scratch_shapes=[
            pltpu.VMEM(probe.shape, f32),
            pltpu.VMEM(raw_counts.shape, bf16),
            pltpu.VMEM(delta.shape, f32),
            pltpu.VMEM(forward.shape, bf16),
            pltpu.VMEM(backward.shape, bf16),
            pltpu.VMEM((2, reach, reach), f32),
            pltpu.VMEM((rows, points, points), bf16),
            pltpu.VMEM((rows, points, points), bf16),
            pltpu.VMEM((rows, 8, 128), i32),
            pltpu.VMEM((rows, 8, 128), i32),
            pltpu.SMEM((rows, 8, 128), i32),
            pltpu.VMEM((rows, 2, points, points), f32),
            pltpu.VMEM((rows, modes, points, 2 * points), bf16),
            pltpu.VMEM((modes, points, 2 * points), f32),
            pltpu.VMEM((rows, 2, points, points), f32),
            pltpu.VMEM((modes, length, points), f32),
            pltpu.VMEM((WAYS if rows <= 8 else 1, 2 * tile + points, 2 * tile + half), f32),
            pltpu.VMEM((2, 2, tile, half), i16),
            pltpu.VMEM((2, 2, half, tile), i16),
            pltpu.VMEM((4, 2, half, half), i16),
            pltpu.VMEM((2, 2, tile, half), i16),
            pltpu.VMEM((2, 2, half, tile), i16),
            pltpu.VMEM((4, 2, half, half), i16),
            pltpu.VMEM((8, 128), f32),
            pltpu.VMEM((8, 8, 128), f32),
            pltpu.VMEM((modes, length, lanes), f32),
            pltpu.VMEM((modes, length, lanes), f32),
            pltpu.VMEM((modes * chips, length // chips, lanes), f32),
            pltpu.VMEM((modes, length // chips, lanes), f32),
            pltpu.VMEM((modes * cols, length // chips // cols, lanes), f32),
            pltpu.VMEM((modes, length // chips // cols, lanes), f32),
            pltpu.VMEM((modes, length // chips, lanes), f32),
            pltpu.VMEM((modes, length, lanes), f32),
            dma((7,)),
            dma((8,)),
            dma((8,)),
            dma((rows,)),
            dma((rows,)),
            dma((rows,)),
            dma((rows,)),
            dma((2, 8)),
            dma((2, 8)),
            dma((8,)),
            dma((8,)),
            dma((2, modes)),
            dma((2, modes * chips)),
            dma((2, modes * cols)),
            dma((2, modes * cols)),
            dma((2, modes * chips)),
            dma((2, modes)),
        ],
        compiler_params=pltpu.CompilerParams(
            collective_id=0, has_side_effects=True, vmem_limit_bytes=67043328
        ),
    )(tile_row, offsets, object_field, probe, raw_counts, delta, forward, backward)


def shards(object_field, probe, raw_counts, resample_delta, tile_row, offsets):
    points = probe.shape[-1]
    frame_total = raw_counts.shape[0] * lax.axis_size("row") * lax.axis_size("col")
    forward, backward = dft_tables(points)
    object_grad, summed = whole(
        tile_row, offsets, object_field, probe, raw_counts, resample_delta, forward, backward
    )
    return (object_grad, summed.reshape(probe.shape) * (1.0 / math.sqrt(frame_total)))


def solution(mesh):
    placed = (
        P(None, "row", "col"),
        P(),
        P(("row", "col"), None, None),
        P(),
        P(("row", "col"), None),
        P(("row", "col"), None),
    )
    return jax.shard_map(
        shards, mesh=mesh, in_specs=placed, out_specs=(P(None, "row", "col"), P()), check_vma=False
    )
```

```python
import math

import jax
import jax.numpy as jnp
import numpy as np
from jax import lax
from jax.experimental import pallas as pl
from jax.experimental.pallas import tpu as pltpu
from jax.sharding import PartitionSpec as P


MESH = pl.DeviceIdType.MESH
GROUP = 2
WAYS = 4
DIRECTIONS = tuple(
    (down, across) for down in (-1, 0, 1) for across in (-1, 0, 1) if (down, across) != (0, 0)
)


def place():
    return (
        lax.axis_index("row"),
        lax.axis_index("col"),
        lax.axis_size("row"),
        lax.axis_size("col"),
    )


def inside(row, col, rows, cols):
    return (row >= 0) & (row < rows) & (col >= 0) & (col < cols)


def inner_edge(step, tile, half):
    start, size = {-1: (0, half), 0: (0, tile), 1: (tile - half, half)}[step]
    return pl.ds(start, size)


def outer_edge(step, tile, half):
    start, size = {-1: (0, half), 0: (half, tile), 1: (half + tile, half)}[step]
    return pl.ds(start, size)


LEVELS = 32767.0


def coded(value, bound):
    level = jnp.sqrt(jnp.abs(value) * (1.0 / bound)) * LEVELS
    level = jnp.where(value < 0.0, -level, level)
    return jnp.round(level).astype(jnp.int32).astype(jnp.int16)


def decoded(code, bound):
    level = code.astype(jnp.int32).astype(jnp.float32) * (1.0 / LEVELS)
    return level * jnp.abs(level) * bound


def greatest(value):
    return jnp.maximum(jnp.max(jnp.abs(value)), 1e-30)


def greet():
    row, col, rows, cols = place()
    barrier = pltpu.get_barrier_semaphore()
    others = [(lax.rem(row + i, rows), col) for i in range(1, rows)]
    others += [(row, lax.rem(col + i, cols)) for i in range(1, cols)]
    for down in (1, rows - 1):
        for across in (1, cols - 1):
            others.append((lax.rem(row + down, rows), lax.rem(col + across, cols)))
    for other in others:
        pl.semaphore_signal(barrier, inc=1, device_id=other, device_id_type=MESH)
    pl.semaphore_wait(barrier, len(others))


def product(left, right):
    return jnp.dot(left, right, preferred_element_type=jnp.float32)


def dft_tables(points):
    indices = np.arange(points)
    angles = (indices[:, None] * indices[None, :] % points) * (2.0 * math.pi / points)
    cosine = np.cos(angles) / math.sqrt(points)
    sine_part = -np.sin(angles) / math.sqrt(points)
    forward = np.block([[cosine, -sine_part], [sine_part, cosine]])
    backward = np.block([[cosine, sine_part], [-sine_part, cosine]])
    return (jnp.asarray(forward, jnp.bfloat16), jnp.asarray(backward, jnp.bfloat16))


def whole_kernel(
    tile_row,
    offsets,
    object_hbm,
    probe_hbm,
    raw_hbm,
    delta_hbm,
    forward_hbm,
    backward_hbm,
    folded,
    summed,
    probe,
    raw,
    delta,
    forward,
    backward,
    extended,
    incoming,
    outbox,
    infos,
    info_out,
    places,
    windows,
    residuals,
    far_field,
    terms,
    total,
    shifted,
    code_tall,
    code_wide,
    code_corners,
    halos_tall,
    halos_wide,
    corners,
    bound_out,
    bounds,
    pair_in,
    pair_sum,
    chip_in,
    chip_sum,
    line_in,
    line_sum,
    line_out,
    chip_out,
    local_sems,
    object_send,
    object_recv,
    relay_sems,
    slot_send,
    slot_recv,
    info_send,
    info_recv,
    halo_send,
    halo_recv,
    bound_send,
    bound_recv,
    pair_sems,
    chip_sems,
    line_sems,
    back_line_sems,
    back_chip_sems,
    back_pair_sems,
):
    row, col, rows, cols = place()
    tile = folded.shape[1]
    points = raw.shape[1]
    half = points // 2
    reach = tile + points
    mode_count = probe.shape[0]
    frame_count = raw.shape[0]
    gradient = extended

    loads = [
        pltpu.make_async_copy(source, target, local_sems.at[i])
        for i, (source, target) in enumerate(
            (
                (raw_hbm, raw),
                (delta_hbm, delta),
                (object_hbm, extended.at[:, pl.ds(half, tile), pl.ds(half, tile)]),
                (probe_hbm, probe),
                (forward_hbm, forward),
                (backward_hbm, backward),
            )
        )
    ]
    for load in loads:
        load.start()
    greet()

    lanes_of = lax.broadcasted_iota(jnp.int32, (8, 128), 1)

    def chosen(other):
        pick, top, left, live = (jnp.int32(0), jnp.int32(0), jnp.int32(0), jnp.int32(0))
        for k in range(frame_count):
            hit = tile_row[k, 0] == other
            pick = jnp.where(hit, k, pick)
            top = jnp.where(hit, offsets[k, 0], top)
            left = jnp.where(hit, offsets[k, 1], left)
            live = jnp.where(hit, 1, live)
        return pick, top, left, live

    def info_copy(step, target, other):
        return pltpu.make_async_remote_copy(
            src_ref=info_out.at[step],
            dst_ref=infos.at[target],
            send_sem=info_send.at[step],
            recv_sem=info_recv.at[target],
            device_id=(other, col),
            device_id_type=MESH,
        )

    def slot_copy(step, target, other):
        return pltpu.make_async_remote_copy(
            src_ref=outbox.at[step],
            dst_ref=incoming.at[target],
            send_sem=slot_send.at[step],
            recv_sem=slot_recv.at[target],
            device_id=(other, col),
            device_id_type=MESH,
        )

    def tell(step, carry):
        other = lax.rem(row + step, rows)
        _, top, left, live = chosen(other)
        info = jnp.where(lanes_of == 0, top, jnp.where(lanes_of == 1, left, live))

        @pl.when(step == 0)
        def _():
            infos[row] = info

        @pl.when(step > 0)
        def _():
            info_out[step] = info
            info_copy(step, row, other).start()

        return carry

    lax.fori_loop(0, rows, tell, 0)

    def pick(tall, wide, corner, index, part):
        down, across = DIRECTIONS[index]
        if down and across:
            return corner.at[(down + 1) + (across + 1) // 2, part]
        return wide.at[(down + 1) // 2, part] if down else tall.at[(across + 1) // 2, part]

    def bound_copy(index, part):
        down, across = DIRECTIONS[index]
        return pltpu.make_async_remote_copy(
            src_ref=bound_out.at[part],
            dst_ref=bounds.at[part, index],
            send_sem=bound_send.at[part, index],
            recv_sem=bound_recv.at[part, index],
            device_id=(row + down, col + across),
            device_id_type=MESH,
        )

    def object_halo(index):
        down, across = DIRECTIONS[index]
        return pltpu.make_async_remote_copy(
            src_ref=object_hbm.at[
                :, inner_edge(down, tile, half), inner_edge(across, tile, half)
            ],
            dst_ref=extended.at[
                :, outer_edge(-down, tile, half), outer_edge(-across, tile, half)
            ],
            send_sem=object_send.at[index],
            recv_sem=object_recv.at[index],
            device_id=(row + down, col + across),
            device_id_type=MESH,
        )

    for index, (down, across) in enumerate(DIRECTIONS):

        if not (down and across):

            @pl.when(inside(row + down, col + across, rows, cols))
            def _():
                object_halo(index).start()

        @pl.when(jnp.logical_not(inside(row - down, col - across, rows, cols)))
        def _():
            where = (slice(None), outer_edge(-down, tile, half), outer_edge(-across, tile, half))
            extended[where] = jnp.zeros((2, where[1].size, where[2].size), jnp.float32)

    core = lax.rem(row, 2)
    near = 1 - 2 * core
    sides = ((0, -1), (1, 1))

    def pair_relay(side, across):
        source = pl.multiple_of(tile * (1 - core) + half * core, 8)
        target = pl.multiple_of((half + tile) * core, 8)
        lanes_at = outer_edge(across, tile, half)
        return pltpu.make_async_remote_copy(
            src_ref=extended.at[:, pl.ds(source, half), lanes_at],
            dst_ref=extended.at[:, pl.ds(target, half), lanes_at],
            send_sem=relay_sems.at[0, 0, side],
            recv_sem=relay_sems.at[0, 1, side],
            device_id=(row + near, col),
            device_id_type=MESH,
        )

    def line_relay(side, across):
        rows_at = pl.ds(pl.multiple_of((half + tile) * core, 8), half)
        return pltpu.make_async_remote_copy(
            src_ref=extended.at[:, rows_at, pl.ds(tile if across > 0 else half, half)],
            dst_ref=extended.at[:, rows_at, outer_edge(-across, tile, half)],
            send_sem=relay_sems.at[1, 0, side],
            recv_sem=relay_sems.at[1, 1, side],
            device_id=(row, col + across),
            device_id_type=MESH,
        )

    def relayed(act_pair, act_line, sending):
        for side, across in sides:

            @pl.when(inside(row, col + across, rows, cols))
            def _():
                act_pair(pair_relay(side, across))

            toward = across if sending else -across

            @pl.when(inside(row - near, col + toward, rows, cols))
            def _():
                act_line(line_relay(side, across))

    loads[0].wait()
    loads[1].wait()
    identity = (
        lax.broadcasted_iota(jnp.int32, (points, points), 0)
        == lax.broadcasted_iota(jnp.int32, (points, points), 1)
    ).astype(jnp.float32)
    resample = (identity + delta[...]).astype(jnp.bfloat16)

    def measure(step, carry):
        other = lax.rem(row + step, rows)
        pick, _, _, _ = chosen(other)
        first = product(resample, raw[pick]).astype(jnp.bfloat16)
        second = lax.dot_general(
            first, resample, (((1,), (1,)), ((), ())), preferred_element_type=jnp.float32
        )
        amplitude = jnp.sqrt(jnp.maximum(second, 0.0)).astype(jnp.bfloat16)

        @pl.when(step == 0)
        def _():
            incoming[row] = amplitude

        @pl.when(step > 0)
        def _():
            outbox[step] = amplitude
            slot_copy(step, row, other).start()

        return carry

    lax.fori_loop(0, rows, measure, 0)

    def heard(step, carry):
        source = lax.rem(row - step + rows, rows)
        info_copy(step, source, source).wait()
        return carry

    lax.fori_loop(1, rows, heard, 0)
    noted = pltpu.make_async_copy(infos, places, local_sems.at[6])
    noted.start()
    total[...] = jnp.zeros_like(total)
    shifted[...] = jnp.zeros_like(shifted)
    for side, across in sides:

        @pl.when(inside(row, col + across, rows, cols))
        def _():
            object_halo(DIRECTIONS.index((0, -across))).wait_recv()
            pair_relay(side, across).start()

    for which in range(2):
        far = 2 * which - 1

        @pl.when((core == which) & inside(row + far, col, rows, cols))
        def _():
            object_halo(DIRECTIONS.index((-far, 0))).wait_recv()

    for side, across in sides:

        @pl.when(inside(row - near, col + across, rows, cols))
        def _():
            line_relay(side, across).start()

    for which in range(2):

        @pl.when(core == which)
        def _():
            object_halo(DIRECTIONS.index((2 * which - 1, 0))).wait_recv()

    for load in loads[2:]:
        load.wait()
    noted.wait()
    relayed(lambda copy: copy.wait_recv(), lambda copy: copy.wait_recv(), False)

    span_rows, span_cols = (points + 8, points + 128)

    def spot(step):
        source = lax.rem(row - step + rows, rows)
        return source, places[source, 0, 0], places[source, 0, 1], places[source, 0, 2]

    def onward(step, carry):
        source, top, left, live = spot(step)
        skip_rows, skip_cols = (lax.rem(top, 8), lax.rem(left, 128))
        across_rows = pl.ds(lax.div(top, 8) * 8, span_rows)
        across_cols = pl.ds(lax.div(left, 128) * 128, span_cols)
        for part in range(2):
            block = extended[part, across_rows, across_cols]
            block = pltpu.roll(block, lax.rem(span_cols - skip_cols, span_cols), 1)
            block = block[:, :points]
            block = pltpu.roll(block, lax.rem(span_rows - skip_rows, span_rows), 0)
            windows[step, part] = block[:points]
        intensity = jnp.zeros((points, points), jnp.float32)
        halves = []
        for mode in range(mode_count):
            object_real, object_imag = (windows[step, 0], windows[step, 1])
            probe_real, probe_imag = (probe[mode, 0], probe[mode, 1])
            wave = jnp.concatenate(
                [
                    (probe_real * object_real - probe_imag * object_imag).astype(jnp.bfloat16),
                    (probe_real * object_imag + probe_imag * object_real).astype(jnp.bfloat16),
                ],
                0,
            )
            halves.append(product(forward[...], wave).astype(jnp.bfloat16))
        for mode, half_done in enumerate(halves):
            wave_rows = jnp.concatenate([half_done[:points], half_done[points:]], 1)
            field = product(wave_rows, backward[...])
            far_field[mode] = field
            squares = field * field
            intensity = intensity + squares[:, :points] + squares[:, points:]

        @pl.when(step > 0)
        def _():
            slot_copy(step, source, source).wait_recv()

        amplitude = incoming[source].astype(jnp.float32)
        scaling = 1.0 - amplitude / jnp.sqrt(jnp.maximum(intensity, 1.0))
        scaling = scaling * live.astype(jnp.float32)
        scaling = jnp.concatenate([scaling, scaling], 1)
        for mode in range(mode_count):
            residuals[step, mode] = (far_field[mode] * scaling).astype(jnp.bfloat16)
        return carry

    lax.fori_loop(0, rows, onward, 0)

    def back(mode, group, middle, hook):
        def one(index, carry):
            steps = [index * group + k for k in range(group)]
            backs = [
                product(residuals[step, mode], forward[...]).astype(jnp.bfloat16)
                for step in steps
            ]
            updates = [
                product(
                    backward[...], jnp.concatenate([rows_[:, :points], rows_[:, points:]], 0)
                )
                for rows_ in backs
            ]
            sum_real = total[mode, :points]
            sum_imag = total[mode, points:]
            for step, update in zip(steps, updates):
                update_real, update_imag = (update[:points], update[points:])
                object_real, object_imag = (windows[step, 0], windows[step, 1])
                probe_real, probe_imag = (probe[mode, 0], probe[mode, 1])
                term_real = probe_real * update_real + probe_imag * update_imag
                term_imag = probe_real * update_imag - probe_imag * update_real
                if mode == 0:
                    terms[step, 0] = term_real
                    terms[step, 1] = term_imag
                else:
                    terms[step, 0] += term_real
                    terms[step, 1] += term_imag
                sum_real = sum_real + (object_real * update_real + object_imag * update_imag)
                sum_imag = sum_imag + (object_real * update_imag - object_imag * update_real)
            total[mode, :points] = sum_real
            total[mode, points:] = sum_imag
            if hook:

                @pl.when(index == middle)
                def _():
                    for piece in hook:
                        advance(piece)

            return carry

        return one

    ways = shifted.shape[0]

    def accumulate(part, group):
        chunk = 32
        first = group * ways
        found = [spot(first + k) for k in range(ways)]
        bases = [tile // 8 - lax.div(top, 8) for _, top, _, _ in found]
        acrosses = [(tile // 128 - 1 - lax.div(left, 128)) * 128 for _, _, left, _ in found]
        for k in range(ways):
            _, top, left, _ = found[k]
            block = jnp.concatenate(
                [terms[first + k, part], jnp.zeros((8, points), jnp.float32)], 0
            )
            block = pltpu.roll(block, lax.rem(top, 8), 0)
            block = jnp.concatenate([block, jnp.zeros((span_rows, 128), jnp.float32)], 1)
            shifted[k, pl.ds(tile, span_rows), pl.ds(tile - 128, span_cols)] = pltpu.roll(
                block, lax.rem(left, 128), 1
            )

        def add(index, inner):
            start = pl.multiple_of(index * chunk, 8)
            value = gradient[part, pl.ds(start, chunk)]
            for k in range(ways):
                source = (bases[k] + index * (chunk // 8)) * 8
                value = value + shifted[k, pl.ds(source, chunk), pl.ds(acrosses[k], reach)]
            gradient[part, pl.ds(start, chunk)] = value
            return inner

        lax.fori_loop(0, reach // chunk, add, 0)

    pieces = pair_in.shape[0]
    length = pair_in.shape[1]
    chips = rows // 2
    chip = row // 2
    chip_rows = length // chips
    line_rows = chip_rows // cols
    lanes = summed.shape[2] // 2

    def own_half():
        return pl.ds(pl.multiple_of(core * lanes, lanes), lanes)

    def sibling_half():
        return pl.ds(pl.multiple_of((1 - core) * lanes, lanes), lanes)

    sibling = (row + 1 - 2 * core, col)
    def halo(index, part):
        down, across = DIRECTIONS[index]
        return pltpu.make_async_remote_copy(
            src_ref=pick(code_tall, code_wide, code_corners, index, part),
            dst_ref=pick(halos_tall, halos_wide, corners, index, part),
            send_sem=halo_send.at[part, index],
            recv_sem=halo_recv.at[part, index],
            device_id=(row + down, col + across),
            device_id_type=MESH,
        )

    def encode(part, bound):
        for index, (down, across) in enumerate(DIRECTIONS):
            where = (part, outer_edge(down, tile, half), outer_edge(across, tile, half))
            pick(code_tall, code_wide, code_corners, index, part)[...] = coded(
                gradient[where], bound
            )

    def start_halos(part):
        for index, (down, across) in enumerate(DIRECTIONS):

            @pl.when(inside(row + down, col + across, rows, cols))
            def _():
                bound_copy(index, part).start()
                halo(index, part).start()

    def take_halos(part):
        for index, (down, across) in enumerate(DIRECTIONS):

            @pl.when(inside(row - down, col - across, rows, cols))
            def _():
                bound_copy(index, part).wait_recv()
                halo(index, part).wait_recv()
                where = (part, inner_edge(-down, tile, half), inner_edge(-across, tile, half))
                folded[where] += decoded(
                    pick(halos_tall, halos_wide, corners, index, part)[...],
                    jnp.max(bounds[part, index]),
                )

    def remote(source, target, sems, index, device):
        return pltpu.make_async_remote_copy(
            src_ref=source,
            dst_ref=target,
            send_sem=sems.at[0, index],
            recv_sem=sems.at[1, index],
            device_id=device,
            device_id_type=MESH,
        )

    def pair_copy(piece):
        return remote(
            total.at[piece, :, sibling_half()], pair_in.at[piece], pair_sems, piece, sibling
        )

    def chip_copy(piece, step):
        other = lax.rem(chip + step, chips)
        start = pl.multiple_of(other * chip_rows, 8)
        index = piece * chips + step
        return remote(
            pair_sum.at[piece, pl.ds(start, chip_rows)],
            chip_in.at[index],
            chip_sems,
            index,
            (2 * other + core, col),
        )

    def line_copy(piece, step):
        other = lax.rem(col + step, cols)
        start = pl.multiple_of(other * line_rows, 8)
        index = piece * cols + step
        return remote(
            chip_sum.at[piece, pl.ds(start, line_rows)],
            line_in.at[index],
            line_sems,
            index,
            (row, other),
        )

    def back_line_copy(piece, step):
        other = lax.rem(col + step, cols)
        start = pl.multiple_of(col * line_rows, 8)
        return remote(
            line_sum.at[piece],
            line_out.at[piece, pl.ds(start, line_rows)],
            back_line_sems,
            piece * cols + step,
            (row, other),
        )

    def back_chip_copy(piece, step):
        other = lax.rem(chip + step, chips)
        start = pl.multiple_of(chip * chip_rows, 8)
        return remote(
            line_out.at[piece],
            chip_out.at[piece, pl.ds(start, chip_rows)],
            back_chip_sems,
            piece * chips + step,
            (2 * other + core, col),
        )

    def back_pair_copy(piece):
        return remote(
            chip_out.at[piece],
            summed.at[piece, :, own_half()],
            back_pair_sems,
            piece,
            sibling,
        )

    def pair_stage(piece):
        pair_copy(piece).wait_recv()
        pair_sum[piece] = total[piece, :, own_half()] + pair_in[piece]
        for step in range(1, chips):
            chip_copy(piece, step).start()

    def chip_stage(piece):
        start = pl.multiple_of(chip * chip_rows, 8)
        value = pair_sum[piece, pl.ds(start, chip_rows)]
        for step in range(1, chips):
            chip_copy(piece, step).wait_recv()
            value = value + chip_in[piece * chips + step]
        chip_sum[piece] = value
        for step in range(1, cols):
            line_copy(piece, step).start()

    def line_stage(piece):
        start = pl.multiple_of(col * line_rows, 8)
        value = chip_sum[piece, pl.ds(start, line_rows)]
        for step in range(1, cols):
            line_copy(piece, step).wait_recv()
            value = value + line_in[piece * cols + step]
        line_sum[piece] = value
        line_out[piece, pl.ds(start, line_rows)] = value
        for step in range(1, cols):
            back_line_copy(piece, step).start()

    def back_line_stage(piece):
        for step in range(1, cols):
            back_line_copy(piece, step).wait_recv()
        start = pl.multiple_of(chip * chip_rows, 8)
        for step in range(1, chips):
            back_chip_copy(piece, step).start()
        chip_out[piece, pl.ds(start, chip_rows)] = line_out[piece]

    def back_chip_stage(piece):
        for step in range(1, chips):
            back_chip_copy(piece, step).wait_recv()
        back_pair_copy(piece).start()
        summed[piece, :, own_half()] = chip_out[piece]

    stages = (pair_stage, chip_stage, line_stage, back_line_stage, back_chip_stage)
    reached = [0] * pieces

    def advance(piece):
        if reached[piece] < len(stages):
            stages[reached[piece]](piece)
            reached[piece] += 1

    middle = rows // 2 // GROUP - 1
    for mode in range(mode_count):
        hook = tuple(range(mode))
        lax.fori_loop(0, rows // GROUP, back(mode, GROUP, middle, hook), 0)
        pair_copy(mode).start()

    for index, (down, across) in enumerate(DIRECTIONS):

        if not (down and across):

            @pl.when(inside(row + down, col + across, rows, cols))
            def _():
                object_halo(index).wait_send()

    relayed(lambda copy: copy.wait_send(), lambda copy: copy.wait_send(), True)

    gradient[...] = jnp.zeros_like(gradient)
    passes = rows // ways
    for part, which in enumerate(((0, 1, 2), (0, 1, 2))):
        for group in range(passes):
            accumulate(part, group)
            if group == (passes - 1) // 2:
                for piece in which:
                    advance(piece)
        bound = greatest(gradient[part])
        bound_out[part] = jnp.full((8, 128), bound, jnp.float32)
        encode(part, bound)
        if part == 0:
            start_halos(0)
    advance(1)
    advance(2)
    start_halos(1)
    advance(0)
    folded[...] = gradient[:, half : half + tile, half : half + tile]
    advance(2)
    take_halos(0)
    for _ in stages:
        for piece in range(pieces):
            advance(piece)
    take_halos(1)
    for piece in range(pieces):
        back_pair_copy(piece).wait_recv()
    for index, (down, across) in enumerate(DIRECTIONS):

        @pl.when(inside(row + down, col + across, rows, cols))
        def _():
            bound_copy(index, 0).wait_send()
            bound_copy(index, 1).wait_send()
            halo(index, 0).wait_send()
            halo(index, 1).wait_send()

    def sent(step, carry):
        slot_copy(step, row, lax.rem(row + step, rows)).wait_send()
        return carry

    lax.fori_loop(1, rows, sent, 0)
    for piece in range(pieces):
        pair_copy(piece).wait_send()
        back_pair_copy(piece).wait_send()
        for step in range(1, chips):
            chip_copy(piece, step).wait_send()
            back_chip_copy(piece, step).wait_send()
        for step in range(1, cols):
            line_copy(piece, step).wait_send()
            back_line_copy(piece, step).wait_send()


def whole(tile_row, offsets, object_field, probe, raw_counts, delta, forward, backward):
    rows, cols = (lax.axis_size("row"), lax.axis_size("col"))
    tile = object_field.shape[1]
    modes, _, points, _ = probe.shape
    half = points // 2
    reach = tile + points
    length, lanes = (2 * points, points // 2)
    chips = rows // 2
    f32, bf16, i32, i16 = (jnp.float32, jnp.bfloat16, jnp.int32, jnp.int16)
    vmem = pl.BlockSpec(memory_space=pltpu.VMEM)
    hbm = pl.BlockSpec(memory_space=pl.ANY)
    dma = pltpu.SemaphoreType.DMA
    return pl.pallas_call(
        whole_kernel,
        name="whole",
        out_shape=(
            jax.ShapeDtypeStruct((2, tile, tile), f32),
            jax.ShapeDtypeStruct((modes, length, points), f32),
        ),
        in_specs=[pl.BlockSpec(memory_space=pltpu.SMEM)] * 2 + [hbm] * 6,
        out_specs=(vmem, vmem),
        scratch_shapes=[
            pltpu.VMEM(probe.shape, f32),
            pltpu.VMEM(raw_counts.shape, bf16),
            pltpu.VMEM(delta.shape, f32),
            pltpu.VMEM(forward.shape, bf16),
            pltpu.VMEM(backward.shape, bf16),
            pltpu.VMEM((2, reach, reach), f32),
            pltpu.VMEM((rows, points, points), bf16),
            pltpu.VMEM((rows, points, points), bf16),
            pltpu.VMEM((rows, 8, 128), i32),
            pltpu.VMEM((rows, 8, 128), i32),
            pltpu.SMEM((rows, 8, 128), i32),
            pltpu.VMEM((rows, 2, points, points), f32),
            pltpu.VMEM((rows, modes, points, 2 * points), bf16),
            pltpu.VMEM((modes, points, 2 * points), f32),
            pltpu.VMEM((rows, 2, points, points), f32),
            pltpu.VMEM((modes, length, points), f32),
            pltpu.VMEM((WAYS if rows <= 8 else 1, 2 * tile + points, 2 * tile + half), f32),
            pltpu.VMEM((2, 2, tile, half), i16),
            pltpu.VMEM((2, 2, half, tile), i16),
            pltpu.VMEM((4, 2, half, half), i16),
            pltpu.VMEM((2, 2, tile, half), i16),
            pltpu.VMEM((2, 2, half, tile), i16),
            pltpu.VMEM((4, 2, half, half), i16),
            pltpu.VMEM((2, 8, 128), f32),
            pltpu.VMEM((2, 8, 8, 128), f32),
            pltpu.VMEM((modes, length, lanes), f32),
            pltpu.VMEM((modes, length, lanes), f32),
            pltpu.VMEM((modes * chips, length // chips, lanes), f32),
            pltpu.VMEM((modes, length // chips, lanes), f32),
            pltpu.VMEM((modes * cols, length // chips // cols, lanes), f32),
            pltpu.VMEM((modes, length // chips // cols, lanes), f32),
            pltpu.VMEM((modes, length // chips, lanes), f32),
            pltpu.VMEM((modes, length, lanes), f32),
            dma((7,)),
            dma((8,)),
            dma((8,)),
            dma((2, 2, 2)),
            dma((rows,)),
            dma((rows,)),
            dma((rows,)),
            dma((rows,)),
            dma((2, 8)),
            dma((2, 8)),
            dma((2, 8)),
            dma((2, 8)),
            dma((2, modes)),
            dma((2, modes * chips)),
            dma((2, modes * cols)),
            dma((2, modes * cols)),
            dma((2, modes * chips)),
            dma((2, modes)),
        ],
        compiler_params=pltpu.CompilerParams(
            collective_id=0, has_side_effects=True, vmem_limit_bytes=67043328
        ),
    )(tile_row, offsets, object_field, probe, raw_counts, delta, forward, backward)


def shards(object_field, probe, raw_counts, resample_delta, tile_row, offsets):
    points = probe.shape[-1]
    frame_total = raw_counts.shape[0] * lax.axis_size("row") * lax.axis_size("col")
    forward, backward = dft_tables(points)
    object_grad, summed = whole(
        tile_row, offsets, object_field, probe, raw_counts, resample_delta, forward, backward
    )
    return (object_grad, summed.reshape(probe.shape) * (1.0 / math.sqrt(frame_total)))


def solution(mesh):
    placed = (
        P(None, "row", "col"),
        P(),
        P(("row", "col"), None, None),
        P(),
        P(("row", "col"), None),
        P(("row", "col"), None),
    )
    return jax.shard_map(
        shards, mesh=mesh, in_specs=placed, out_specs=(P(None, "row", "col"), P()), check_vma=False
    )
```

```python
import math

import jax
import jax.numpy as jnp
import numpy as np
from jax import lax
from jax.experimental import pallas as pl
from jax.experimental.pallas import tpu as pltpu
from jax.sharding import PartitionSpec as P


MESH = pl.DeviceIdType.MESH
GROUP = 2
WAYS = 4
DIRECTIONS = tuple(
    (down, across) for down in (-1, 0, 1) for across in (-1, 0, 1) if (down, across) != (0, 0)
)


def place():
    return (
        lax.axis_index("row"),
        lax.axis_index("col"),
        lax.axis_size("row"),
        lax.axis_size("col"),
    )


def inside(row, col, rows, cols):
    return (row >= 0) & (row < rows) & (col >= 0) & (col < cols)


def inner_edge(step, tile, half):
    start, size = {-1: (0, half), 0: (0, tile), 1: (tile - half, half)}[step]
    return pl.ds(start, size)


def outer_edge(step, tile, half):
    start, size = {-1: (0, half), 0: (half, tile), 1: (half + tile, half)}[step]
    return pl.ds(start, size)


LEVELS = 32767.0


def coded(value, bound):
    level = jnp.sqrt(jnp.abs(value) * (1.0 / bound)) * LEVELS
    level = jnp.where(value < 0.0, -level, level)
    return jnp.round(level).astype(jnp.int32).astype(jnp.int16)


def decoded(code, bound):
    level = code.astype(jnp.int32).astype(jnp.float32) * (1.0 / LEVELS)
    return level * jnp.abs(level) * bound


def greatest(value):
    return jnp.maximum(jnp.max(jnp.abs(value)), 1e-30)


def greet():
    row, col, rows, cols = place()
    barrier = pltpu.get_barrier_semaphore()
    others = [(lax.rem(row + i, rows), col) for i in range(1, rows)]
    others += [(row, lax.rem(col + i, cols)) for i in range(1, cols)]
    for down in (1, rows - 1):
        for across in (1, cols - 1):
            others.append((lax.rem(row + down, rows), lax.rem(col + across, cols)))
    for other in others:
        pl.semaphore_signal(barrier, inc=1, device_id=other, device_id_type=MESH)
    pl.semaphore_wait(barrier, len(others))


def product(left, right):
    return jnp.dot(left, right, preferred_element_type=jnp.float32)


def dft_tables(points):
    indices = np.arange(points)
    angles = (indices[:, None] * indices[None, :] % points) * (2.0 * math.pi / points)
    cosine = np.cos(angles) / math.sqrt(points)
    sine_part = -np.sin(angles) / math.sqrt(points)
    forward = np.block([[cosine, -sine_part], [sine_part, cosine]])
    backward = np.block([[cosine, sine_part], [-sine_part, cosine]])
    return (jnp.asarray(forward, jnp.bfloat16), jnp.asarray(backward, jnp.bfloat16))


def whole_kernel(
    tile_row,
    offsets,
    object_hbm,
    probe_hbm,
    raw_hbm,
    delta_hbm,
    forward_hbm,
    backward_hbm,
    folded_out,
    summed_out,
    folded,
    summed,
    out_sems,
    probe,
    raw,
    delta,
    forward,
    backward,
    extended,
    incoming,
    outbox,
    infos,
    info_out,
    places,
    windows,
    residuals,
    far_field,
    terms,
    total,
    shifted,
    code_tall,
    code_wide,
    code_corners,
    halos_tall,
    halos_wide,
    corners,
    bound_out,
    bounds,
    pair_in,
    pair_sum,
    chip_in,
    chip_sum,
    line_in,
    line_sum,
    line_out,
    chip_out,
    local_sems,
    object_send,
    object_recv,
    relay_sems,
    slot_send,
    slot_recv,
    info_send,
    info_recv,
    halo_send,
    halo_recv,
    bound_send,
    bound_recv,
    pair_sems,
    chip_sems,
    line_sems,
    back_line_sems,
    back_chip_sems,
    back_pair_sems,
):
    row, col, rows, cols = place()
    tile = folded.shape[1]
    points = raw.shape[1]
    half = points // 2
    reach = tile + points
    mode_count = probe.shape[0]
    frame_count = raw.shape[0]
    gradient = extended

    loads = [
        pltpu.make_async_copy(source, target, local_sems.at[i])
        for i, (source, target) in enumerate(
            (
                (raw_hbm, raw),
                (delta_hbm, delta),
                (object_hbm, extended.at[:, pl.ds(half, tile), pl.ds(half, tile)]),
                (probe_hbm, probe),
                (forward_hbm, forward),
                (backward_hbm, backward),
            )
        )
    ]
    for load in loads:
        load.start()
    greet()

    lanes_of = lax.broadcasted_iota(jnp.int32, (8, 128), 1)

    def chosen(other):
        pick, top, left, live = (jnp.int32(0), jnp.int32(0), jnp.int32(0), jnp.int32(0))
        for k in range(frame_count):
            hit = tile_row[0, k] == other
            pick = jnp.where(hit, k, pick)
            top = jnp.where(hit, offsets[0, k], top)
            left = jnp.where(hit, offsets[1, k], left)
            live = jnp.where(hit, 1, live)
        return pick, top, left, live

    def info_copy(step, target, other):
        return pltpu.make_async_remote_copy(
            src_ref=info_out.at[step],
            dst_ref=infos.at[target],
            send_sem=info_send.at[step],
            recv_sem=info_recv.at[target],
            device_id=(other, col),
            device_id_type=MESH,
        )

    def slot_copy(step, target, other):
        return pltpu.make_async_remote_copy(
            src_ref=outbox.at[step],
            dst_ref=incoming.at[target],
            send_sem=slot_send.at[step],
            recv_sem=slot_recv.at[target],
            device_id=(other, col),
            device_id_type=MESH,
        )

    def tell(step, carry):
        other = lax.rem(row + step, rows)
        _, top, left, live = chosen(other)
        info = jnp.where(lanes_of == 0, top, jnp.where(lanes_of == 1, left, live))

        @pl.when(step == 0)
        def _():
            infos[row] = info

        @pl.when(step > 0)
        def _():
            info_out[step] = info
            info_copy(step, row, other).start()

        return carry

    lax.fori_loop(0, rows, tell, 0)

    def pick(tall, wide, corner, index, part):
        down, across = DIRECTIONS[index]
        if down and across:
            return corner.at[(down + 1) + (across + 1) // 2, part]
        return wide.at[(down + 1) // 2, part] if down else tall.at[(across + 1) // 2, part]

    def bound_copy(index, part):
        down, across = DIRECTIONS[index]
        return pltpu.make_async_remote_copy(
            src_ref=bound_out.at[part],
            dst_ref=bounds.at[part, index],
            send_sem=bound_send.at[part, index],
            recv_sem=bound_recv.at[part, index],
            device_id=(row + down, col + across),
            device_id_type=MESH,
        )

    def object_halo(index):
        down, across = DIRECTIONS[index]
        if down:
            start, size = {-1: (0, half), 0: (half, tile - points), 1: (tile - half, half)}[across]
            lanes_from, lanes_to = (pl.ds(start, size), pl.ds(half + start, size))
            device = (row + down, col)
        else:
            lanes_from = inner_edge(across, tile, half)
            lanes_to = outer_edge(-across, tile, half)
            device = (row, col + across)
        return pltpu.make_async_remote_copy(
            src_ref=object_hbm.at[:, inner_edge(down, tile, half), lanes_from],
            dst_ref=extended.at[:, outer_edge(-down, tile, half), lanes_to],
            send_sem=object_send.at[index],
            recv_sem=object_recv.at[index],
            device_id=device,
            device_id_type=MESH,
        )

    def strips(down):
        return [DIRECTIONS.index((down, across)) for across in (-1, 1, 0)]

    for down in (-1, 1):

        @pl.when(inside(row + down, col, rows, cols))
        def _():
            for index in strips(down):
                object_halo(index).start()

    for across in (-1, 1):

        @pl.when(inside(row, col + across, rows, cols))
        def _():
            object_halo(DIRECTIONS.index((0, across))).start()

    for index, (down, across) in enumerate(DIRECTIONS):

        @pl.when(jnp.logical_not(inside(row - down, col - across, rows, cols)))
        def _():
            where = (slice(None), outer_edge(-down, tile, half), outer_edge(-across, tile, half))
            extended[where] = jnp.zeros((2, where[1].size, where[2].size), jnp.float32)

    core = lax.rem(row, 2)
    near = 1 - 2 * core
    sides = ((0, -1), (1, 1))

    def pair_relay(side, across):
        source = pl.multiple_of(tile * (1 - core) + half * core, 8)
        target = pl.multiple_of((half + tile) * core, 8)
        lanes_at = outer_edge(across, tile, half)
        return pltpu.make_async_remote_copy(
            src_ref=extended.at[:, pl.ds(source, half), lanes_at],
            dst_ref=extended.at[:, pl.ds(target, half), lanes_at],
            send_sem=relay_sems.at[0, 0, side],
            recv_sem=relay_sems.at[0, 1, side],
            device_id=(row + near, col),
            device_id_type=MESH,
        )

    def line_relay(side, across):
        rows_at = pl.ds(pl.multiple_of((half + tile) * core, 8), half)
        return pltpu.make_async_remote_copy(
            src_ref=extended.at[:, rows_at, pl.ds(tile if across > 0 else half, half)],
            dst_ref=extended.at[:, rows_at, outer_edge(-across, tile, half)],
            send_sem=relay_sems.at[1, 0, side],
            recv_sem=relay_sems.at[1, 1, side],
            device_id=(row, col + across),
            device_id_type=MESH,
        )

    def relayed(act_pair, act_line, sending):
        for side, across in sides:

            @pl.when(inside(row, col + across, rows, cols))
            def _():
                act_pair(pair_relay(side, across))

            toward = across if sending else -across

            @pl.when(inside(row - near, col + toward, rows, cols))
            def _():
                act_line(line_relay(side, across))

    loads[0].wait()
    loads[1].wait()
    identity = (
        lax.broadcasted_iota(jnp.int32, (points, points), 0)
        == lax.broadcasted_iota(jnp.int32, (points, points), 1)
    ).astype(jnp.float32)
    resample = (identity + delta[...]).astype(jnp.bfloat16)

    def measure(step, carry):
        other = lax.rem(row + step, rows)
        pick, _, _, _ = chosen(other)
        first = product(resample, raw[pick]).astype(jnp.bfloat16)
        second = lax.dot_general(
            first, resample, (((1,), (1,)), ((), ())), preferred_element_type=jnp.float32
        )
        amplitude = jnp.sqrt(jnp.maximum(second, 0.0)).astype(jnp.bfloat16)

        @pl.when(step == 0)
        def _():
            incoming[row] = amplitude

        @pl.when(step > 0)
        def _():
            outbox[step] = amplitude
            slot_copy(step, row, other).start()

        return carry

    lax.fori_loop(0, rows, measure, 0)

    def heard(step, carry):
        source = lax.rem(row - step + rows, rows)
        info_copy(step, source, source).wait()
        return carry

    lax.fori_loop(1, rows, heard, 0)
    noted = pltpu.make_async_copy(infos, places, local_sems.at[6])
    noted.start()
    total[...] = jnp.zeros_like(total)
    shifted[...] = jnp.zeros_like(shifted)
    for which in range(2):
        far = 2 * which - 1

        @pl.when((core == which) & inside(row + far, col, rows, cols))
        def _():
            for index in strips(-far)[:2]:
                object_halo(index).wait_recv()

    for side, across in sides:

        @pl.when(inside(row - near, col + across, rows, cols))
        def _():
            line_relay(side, across).start()

    for side, across in sides:

        @pl.when(inside(row, col + across, rows, cols))
        def _():
            object_halo(DIRECTIONS.index((0, -across))).wait_recv()
            pair_relay(side, across).start()

    for which in range(2):
        far = 2 * which - 1

        @pl.when((core == which) & inside(row + far, col, rows, cols))
        def _():
            object_halo(strips(-far)[2]).wait_recv()

        @pl.when(core == which)
        def _():
            for index in strips(far):
                object_halo(index).wait_recv()

    for load in loads[2:]:
        load.wait()
    noted.wait()
    relayed(lambda copy: copy.wait_recv(), lambda copy: copy.wait_recv(), False)

    span_rows, span_cols = (points + 8, points + 128)

    def spot(step):
        source = lax.rem(row - step + rows, rows)
        return source, places[source, 0, 0], places[source, 0, 1], places[source, 0, 2]

    def onward(pair, carry):
        steps = [pair * GROUP + k for k in range(GROUP)]
        spots = [spot(step) for step in steps]
        for step, (_, top, left, _) in zip(steps, spots):
            skip_rows, skip_cols = (lax.rem(top, 8), lax.rem(left, 128))
            across_rows = pl.ds(lax.div(top, 8) * 8, span_rows)
            across_cols = pl.ds(lax.div(left, 128) * 128, span_cols)
            for part in range(2):
                block = extended[part, across_rows, across_cols]
                block = pltpu.roll(block, lax.rem(span_cols - skip_cols, span_cols), 1)
                block = block[:, :points]
                block = pltpu.roll(block, lax.rem(span_rows - skip_rows, span_rows), 0)
                windows[step, part] = block[:points]
        halves = []
        for step in steps:
            for mode in range(mode_count):
                object_real, object_imag = (windows[step, 0], windows[step, 1])
                probe_real, probe_imag = (probe[mode, 0], probe[mode, 1])
                wave = jnp.concatenate(
                    [
                        (probe_real * object_real - probe_imag * object_imag).astype(
                            jnp.bfloat16
                        ),
                        (probe_real * object_imag + probe_imag * object_real).astype(
                            jnp.bfloat16
                        ),
                    ],
                    0,
                )
                halves.append(product(forward[...], wave).astype(jnp.bfloat16))
        intensities = []
        for k in range(GROUP):
            intensity = jnp.zeros((points, points), jnp.float32)
            for mode in range(mode_count):
                half_done = halves[k * mode_count + mode]
                wave_rows = jnp.concatenate([half_done[:points], half_done[points:]], 1)
                field = product(wave_rows, backward[...])
                far_field[k, mode] = field
                squares = field * field
                intensity = intensity + squares[:, :points] + squares[:, points:]
            intensities.append(intensity)
        for step, (source, _, _, _) in zip(steps, spots):

            @pl.when(step > 0)
            def _():
                slot_copy(step, source, source).wait_recv()

        for k, (step, (source, _, _, live)) in enumerate(zip(steps, spots)):
            amplitude = incoming[source].astype(jnp.float32)
            scaling = 1.0 - amplitude / jnp.sqrt(jnp.maximum(intensities[k], 1.0))
            scaling = scaling * live.astype(jnp.float32)
            scaling = jnp.concatenate([scaling, scaling], 1)
            for mode in range(mode_count):
                residuals[step, mode] = (far_field[k, mode] * scaling).astype(jnp.bfloat16)
        return carry

    lax.fori_loop(0, rows // GROUP, onward, 0)

    def back(mode, group, middle, hook):
        def one(index, carry):
            steps = [index * group + k for k in range(group)]
            backs = [
                product(residuals[step, mode], forward[...]).astype(jnp.bfloat16)
                for step in steps
            ]
            updates = [
                product(
                    backward[...], jnp.concatenate([rows_[:, :points], rows_[:, points:]], 0)
                )
                for rows_ in backs
            ]
            sum_real = total[mode, :points]
            sum_imag = total[mode, points:]
            for step, update in zip(steps, updates):
                update_real, update_imag = (update[:points], update[points:])
                object_real, object_imag = (windows[step, 0], windows[step, 1])
                probe_real, probe_imag = (probe[mode, 0], probe[mode, 1])
                term_real = probe_real * update_real + probe_imag * update_imag
                term_imag = probe_real * update_imag - probe_imag * update_real
                if mode == 0:
                    terms[step, 0] = term_real
                    terms[step, 1] = term_imag
                else:
                    terms[step, 0] += term_real
                    terms[step, 1] += term_imag
                sum_real = sum_real + (object_real * update_real + object_imag * update_imag)
                sum_imag = sum_imag + (object_real * update_imag - object_imag * update_real)
            total[mode, :points] = sum_real
            total[mode, points:] = sum_imag
            if hook:

                @pl.when(index == middle)
                def _():
                    for piece in hook:
                        advance(piece)

            return carry

        return one

    ways = shifted.shape[0]

    def accumulate(part, group):
        chunk = 32
        first = group * ways
        found = [spot(first + k) for k in range(ways)]
        bases = [tile // 8 - lax.div(top, 8) for _, top, _, _ in found]
        acrosses = [(tile // 128 - 1 - lax.div(left, 128)) * 128 for _, _, left, _ in found]
        for k in range(ways):
            _, top, left, _ = found[k]
            block = jnp.concatenate(
                [terms[first + k, part], jnp.zeros((8, points), jnp.float32)], 0
            )
            block = pltpu.roll(block, lax.rem(top, 8), 0)
            block = jnp.concatenate([block, jnp.zeros((span_rows, 128), jnp.float32)], 1)
            shifted[k, pl.ds(tile, span_rows), pl.ds(tile - 128, span_cols)] = pltpu.roll(
                block, lax.rem(left, 128), 1
            )

        def add(index, inner):
            start = pl.multiple_of(index * chunk, 8)
            value = gradient[part, pl.ds(start, chunk)]
            for k in range(ways):
                source = (bases[k] + index * (chunk // 8)) * 8
                value = value + shifted[k, pl.ds(source, chunk), pl.ds(acrosses[k], reach)]
            gradient[part, pl.ds(start, chunk)] = value
            return inner

        lax.fori_loop(0, reach // chunk, add, 0)

    pieces = pair_in.shape[0]
    length = pair_in.shape[1]
    chips = rows // 2
    chip = row // 2
    norming = 1.0 / math.sqrt(frame_count * rows * cols)

    def folded_copy(part):
        return pltpu.make_async_copy(folded.at[part], folded_out.at[part], out_sems.at[0, part])

    def summed_copy(piece):
        return pltpu.make_async_copy(
            summed.at[piece], summed_out.at[piece], out_sems.at[1, piece]
        )

    chip_rows = length // chips
    line_rows = chip_rows // cols
    lanes = summed.shape[2] // 2

    def own_half():
        return pl.ds(pl.multiple_of(core * lanes, lanes), lanes)

    def sibling_half():
        return pl.ds(pl.multiple_of((1 - core) * lanes, lanes), lanes)

    sibling = (row + 1 - 2 * core, col)
    def halo(index, part):
        down, across = DIRECTIONS[index]
        return pltpu.make_async_remote_copy(
            src_ref=pick(code_tall, code_wide, code_corners, index, part),
            dst_ref=pick(halos_tall, halos_wide, corners, index, part),
            send_sem=halo_send.at[part, index],
            recv_sem=halo_recv.at[part, index],
            device_id=(row + down, col + across),
            device_id_type=MESH,
        )

    def encode(part, bound):
        for index, (down, across) in enumerate(DIRECTIONS):
            where = (part, outer_edge(down, tile, half), outer_edge(across, tile, half))
            pick(code_tall, code_wide, code_corners, index, part)[...] = coded(
                gradient[where], bound
            )

    def start_halos(part, wanted=(-1, 0, 1)):
        for index, (down, across) in enumerate(DIRECTIONS):
            if down not in wanted:
                continue

            @pl.when(inside(row + down, col + across, rows, cols))
            def _():
                bound_copy(index, part).start()
                halo(index, part).start()

    def take_halos(part):
        for index, (down, across) in enumerate(DIRECTIONS):

            @pl.when(inside(row - down, col - across, rows, cols))
            def _():
                bound_copy(index, part).wait_recv()
                halo(index, part).wait_recv()
                where = (part, inner_edge(-down, tile, half), inner_edge(-across, tile, half))
                folded[where] += decoded(
                    pick(halos_tall, halos_wide, corners, index, part)[...],
                    jnp.max(bounds[part, index]),
                )

    def remote(source, target, sems, index, device):
        return pltpu.make_async_remote_copy(
            src_ref=source,
            dst_ref=target,
            send_sem=sems.at[0, index],
            recv_sem=sems.at[1, index],
            device_id=device,
            device_id_type=MESH,
        )

    def pair_copy(piece):
        return remote(
            total.at[piece, :, sibling_half()], pair_in.at[piece], pair_sems, piece, sibling
        )

    def chip_copy(piece, step):
        other = lax.rem(chip + step, chips)
        start = pl.multiple_of(other * chip_rows, 8)
        index = piece * chips + step
        return remote(
            pair_sum.at[piece, pl.ds(start, chip_rows)],
            chip_in.at[index],
            chip_sems,
            index,
            (2 * other + core, col),
        )

    def line_copy(piece, step):
        other = lax.rem(col + step, cols)
        start = pl.multiple_of(other * line_rows, 8)
        index = piece * cols + step
        return remote(
            chip_sum.at[piece, pl.ds(start, line_rows)],
            line_in.at[index],
            line_sems,
            index,
            (row, other),
        )

    def back_line_copy(piece, step):
        other = lax.rem(col + step, cols)
        start = pl.multiple_of(col * line_rows, 8)
        return remote(
            line_sum.at[piece],
            line_out.at[piece, pl.ds(start, line_rows)],
            back_line_sems,
            piece * cols + step,
            (row, other),
        )

    def back_chip_copy(piece, step):
        other = lax.rem(chip + step, chips)
        start = pl.multiple_of(chip * chip_rows, 8)
        return remote(
            line_out.at[piece],
            chip_out.at[piece, pl.ds(start, chip_rows)],
            back_chip_sems,
            piece * chips + step,
            (2 * other + core, col),
        )

    def back_pair_copy(piece):
        return remote(
            chip_out.at[piece],
            summed.at[piece, :, own_half()],
            back_pair_sems,
            piece,
            sibling,
        )

    def pair_stage(piece):
        pair_copy(piece).wait_recv()
        pair_sum[piece] = total[piece, :, own_half()] + pair_in[piece]
        for step in range(1, chips):
            chip_copy(piece, step).start()

    def chip_stage(piece):
        start = pl.multiple_of(chip * chip_rows, 8)
        value = pair_sum[piece, pl.ds(start, chip_rows)]
        for step in range(1, chips):
            chip_copy(piece, step).wait_recv()
            value = value + chip_in[piece * chips + step]
        chip_sum[piece] = value
        for step in range(1, cols):
            line_copy(piece, step).start()

    def line_stage(piece):
        start = pl.multiple_of(col * line_rows, 8)
        value = chip_sum[piece, pl.ds(start, line_rows)]
        for step in range(1, cols):
            line_copy(piece, step).wait_recv()
            value = value + line_in[piece * cols + step]
        value = value * norming
        line_sum[piece] = value
        line_out[piece, pl.ds(start, line_rows)] = value
        for step in range(1, cols):
            back_line_copy(piece, step).start()

    def back_line_stage(piece):
        for step in range(1, cols):
            back_line_copy(piece, step).wait_recv()
        start = pl.multiple_of(chip * chip_rows, 8)
        for step in range(1, chips):
            back_chip_copy(piece, step).start()
        chip_out[piece, pl.ds(start, chip_rows)] = line_out[piece]

    def back_chip_stage(piece):
        for step in range(1, chips):
            back_chip_copy(piece, step).wait_recv()
        back_pair_copy(piece).start()
        summed[piece, :, own_half()] = chip_out[piece]

    stages = (pair_stage, chip_stage, line_stage, back_line_stage, back_chip_stage)
    reached = [0] * pieces

    def advance(piece):
        if reached[piece] < len(stages):
            stages[reached[piece]](piece)
            reached[piece] += 1

    middle = rows // 2 // GROUP - 1
    for mode in range(mode_count):
        hook = (mode - 1,) if mode else ()
        lax.fori_loop(0, rows // GROUP, back(mode, GROUP, middle, hook), 0)
        pair_copy(mode).start()
    advance(0)

    for index, (down, across) in enumerate(DIRECTIONS):

        @pl.when(inside(row + down, col + (0 if down else across), rows, cols))
        def _():
            object_halo(index).wait_send()

    relayed(lambda copy: copy.wait_send(), lambda copy: copy.wait_send(), True)

    gradient[...] = jnp.zeros_like(gradient)
    passes = rows // ways
    for part, which in enumerate(((0, 1, 2), (0, 1, 2))):
        for group in range(passes):
            accumulate(part, group)
            if group == (passes - 1) // 2:
                for piece in which:
                    advance(piece)
        bound = greatest(gradient[part])
        bound_out[part] = jnp.full((8, 128), bound, jnp.float32)
        encode(part, bound)
        if part == 0:
            start_halos(0)
    advance(1)
    advance(2)
    start_halos(1, (0,))
    advance(0)
    folded[...] = gradient[:, half : half + tile, half : half + tile]
    advance(2)
    start_halos(1, (-1, 1))
    take_halos(0)
    folded_copy(0).start()
    for _ in stages:
        for piece in range(pieces):
            advance(piece)
    take_halos(1)
    folded_copy(1).start()
    for piece in range(pieces):
        back_pair_copy(piece).wait_recv()
        summed_copy(piece).start()
    for index, (down, across) in enumerate(DIRECTIONS):

        @pl.when(inside(row + down, col + across, rows, cols))
        def _():
            bound_copy(index, 0).wait_send()
            bound_copy(index, 1).wait_send()
            halo(index, 0).wait_send()
            halo(index, 1).wait_send()

    def sent(step, carry):
        slot_copy(step, row, lax.rem(row + step, rows)).wait_send()
        return carry

    lax.fori_loop(1, rows, sent, 0)
    for piece in range(pieces):
        pair_copy(piece).wait_send()
        back_pair_copy(piece).wait_send()
        for step in range(1, chips):
            chip_copy(piece, step).wait_send()
            back_chip_copy(piece, step).wait_send()
        for step in range(1, cols):
            line_copy(piece, step).wait_send()
            back_line_copy(piece, step).wait_send()
    for part in range(2):
        folded_copy(part).wait()
    for piece in range(pieces):
        summed_copy(piece).wait()


def whole(tile_row, offsets, object_field, probe, raw_counts, delta, forward, backward):
    rows, cols = (lax.axis_size("row"), lax.axis_size("col"))
    tile = object_field.shape[1]
    modes, _, points, _ = probe.shape
    half = points // 2
    reach = tile + points
    length, lanes = (2 * points, points // 2)
    chips = rows // 2
    f32, bf16, i32, i16 = (jnp.float32, jnp.bfloat16, jnp.int32, jnp.int16)
    vmem = pl.BlockSpec(memory_space=pltpu.VMEM)
    hbm = pl.BlockSpec(memory_space=pl.ANY)
    dma = pltpu.SemaphoreType.DMA
    return pl.pallas_call(
        whole_kernel,
        name="whole",
        out_shape=(
            jax.ShapeDtypeStruct((2, tile, tile), f32),
            jax.ShapeDtypeStruct((modes, length, points), f32),
        ),
        in_specs=[pl.BlockSpec(memory_space=pltpu.SMEM)] * 2 + [hbm] * 6,
        out_specs=(hbm, hbm),
        scratch_shapes=[
            pltpu.VMEM((2, tile, tile), f32),
            pltpu.VMEM((modes, length, points), f32),
            dma((2, max(2, modes))),
            pltpu.VMEM(probe.shape, f32),
            pltpu.VMEM(raw_counts.shape, bf16),
            pltpu.VMEM(delta.shape, f32),
            pltpu.VMEM(forward.shape, bf16),
            pltpu.VMEM(backward.shape, bf16),
            pltpu.VMEM((2, reach, reach), f32),
            pltpu.VMEM((rows, points, points), bf16),
            pltpu.VMEM((rows, points, points), bf16),
            pltpu.VMEM((rows, 8, 128), i32),
            pltpu.VMEM((rows, 8, 128), i32),
            pltpu.SMEM((rows, 8, 128), i32),
            pltpu.VMEM((rows, 2, points, points), f32),
            pltpu.VMEM((rows, modes, points, 2 * points), bf16),
            pltpu.VMEM((GROUP, modes, points, 2 * points), f32),
            pltpu.VMEM((rows, 2, points, points), f32),
            pltpu.VMEM((modes, length, points), f32),
            pltpu.VMEM((WAYS if rows <= 8 else 1, 2 * tile + points, 2 * tile + half), f32),
            pltpu.VMEM((2, 2, tile, half), i16),
            pltpu.VMEM((2, 2, half, tile), i16),
            pltpu.VMEM((4, 2, half, half), i16),
            pltpu.VMEM((2, 2, tile, half), i16),
            pltpu.VMEM((2, 2, half, tile), i16),
            pltpu.VMEM((4, 2, half, half), i16),
            pltpu.VMEM((2, 8, 128), f32),
            pltpu.VMEM((2, 8, 8, 128), f32),
            pltpu.VMEM((modes, length, lanes), f32),
            pltpu.VMEM((modes, length, lanes), f32),
            pltpu.VMEM((modes * chips, length // chips, lanes), f32),
            pltpu.VMEM((modes, length // chips, lanes), f32),
            pltpu.VMEM((modes * cols, length // chips // cols, lanes), f32),
            pltpu.VMEM((modes, length // chips // cols, lanes), f32),
            pltpu.VMEM((modes, length // chips, lanes), f32),
            pltpu.VMEM((modes, length, lanes), f32),
            dma((7,)),
            dma((8,)),
            dma((8,)),
            dma((2, 2, 2)),
            dma((rows,)),
            dma((rows,)),
            dma((rows,)),
            dma((rows,)),
            dma((2, 8)),
            dma((2, 8)),
            dma((2, 8)),
            dma((2, 8)),
            dma((2, modes)),
            dma((2, modes * chips)),
            dma((2, modes * cols)),
            dma((2, modes * cols)),
            dma((2, modes * chips)),
            dma((2, modes)),
        ],
        compiler_params=pltpu.CompilerParams(
            collective_id=0, has_side_effects=True, vmem_limit_bytes=67043328
        ),
    )(tile_row, offsets, object_field, probe, raw_counts, delta, forward, backward)


def shards(object_field, probe, raw_counts, resample_delta, tile_row, offsets):
    points = probe.shape[-1]
    forward, backward = dft_tables(points)
    object_grad, summed = whole(
        tile_row.T, offsets.T, object_field, probe, raw_counts, resample_delta, forward, backward
    )
    return (object_grad, summed.reshape(probe.shape))


def solution(mesh):
    placed = (
        P(None, "row", "col"),
        P(),
        P(("row", "col"), None, None),
        P(),
        P(("row", "col"), None),
        P(("row", "col"), None),
    )
    return jax.shard_map(
        shards, mesh=mesh, in_specs=placed, out_specs=(P(None, "row", "col"), P()), check_vma=False
    )
```

```python
import math

import jax
import jax.numpy as jnp
import numpy as np
from jax import lax
from jax.experimental import pallas as pl
from jax.experimental.pallas import tpu as pltpu
from jax.sharding import PartitionSpec as P


MESH = pl.DeviceIdType.MESH
GROUP = 2
BACK_GROUP = 4
WAYS = 4
DIRECTIONS = tuple(
    (down, across) for down in (-1, 0, 1) for across in (-1, 0, 1) if (down, across) != (0, 0)
)


def place():
    return (
        lax.axis_index("row"),
        lax.axis_index("col"),
        lax.axis_size("row"),
        lax.axis_size("col"),
    )


def inside(row, col, rows, cols):
    return (row >= 0) & (row < rows) & (col >= 0) & (col < cols)


def inner_edge(step, tile, half):
    start, size = {-1: (0, half), 0: (0, tile), 1: (tile - half, half)}[step]
    return pl.ds(start, size)


def outer_edge(step, tile, half):
    start, size = {-1: (0, half), 0: (half, tile), 1: (half + tile, half)}[step]
    return pl.ds(start, size)


LEVELS = 32767.0


def coded(value, bound):
    level = jnp.sqrt(jnp.abs(value) * (1.0 / bound)) * LEVELS
    level = jnp.where(value < 0.0, -level, level)
    return jnp.round(level).astype(jnp.int32).astype(jnp.int16)


def decoded(code, bound):
    level = code.astype(jnp.int32).astype(jnp.float32) * (1.0 / LEVELS)
    return level * jnp.abs(level) * bound


def greatest(value):
    return jnp.maximum(jnp.max(jnp.abs(value)), 1e-30)


def greet():
    row, col, rows, cols = place()
    barrier = pltpu.get_barrier_semaphore()
    others = [(lax.rem(row + i, rows), col) for i in range(1, rows)]
    others += [(row, lax.rem(col + i, cols)) for i in range(1, cols)]
    for down in (1, rows - 1):
        for across in (1, cols - 1):
            others.append((lax.rem(row + down, rows), lax.rem(col + across, cols)))
    for other in others:
        pl.semaphore_signal(barrier, inc=1, device_id=other, device_id_type=MESH)
    pl.semaphore_wait(barrier, len(others))


def product(left, right):
    return jnp.dot(left, right, preferred_element_type=jnp.float32)


def dft_tables(points):
    indices = np.arange(points)
    angles = (indices[:, None] * indices[None, :] % points) * (2.0 * math.pi / points)
    cosine = np.cos(angles) / math.sqrt(points)
    sine_part = -np.sin(angles) / math.sqrt(points)
    forward = np.block([[cosine, -sine_part], [sine_part, cosine]])
    backward = np.block([[cosine, sine_part], [-sine_part, cosine]])
    return (jnp.asarray(forward, jnp.bfloat16), jnp.asarray(backward, jnp.bfloat16))


def whole_kernel(
    tile_row,
    offsets,
    object_hbm,
    probe_hbm,
    raw_hbm,
    delta_hbm,
    forward_hbm,
    backward_hbm,
    folded_out,
    summed_out,
    folded,
    summed,
    out_sems,
    probe,
    raw,
    delta,
    forward,
    backward,
    extended,
    incoming,
    outbox,
    infos,
    info_out,
    places,
    windows,
    residuals,
    far_field,
    terms,
    total,
    shifted,
    code_tall,
    code_wide,
    code_corners,
    halos_tall,
    halos_wide,
    corners,
    bound_out,
    bounds,
    pair_in,
    pair_sum,
    chip_in,
    chip_sum,
    line_in,
    line_sum,
    line_out,
    chip_out,
    local_sems,
    object_send,
    object_recv,
    relay_sems,
    slot_send,
    slot_recv,
    info_send,
    info_recv,
    halo_send,
    halo_recv,
    bound_send,
    bound_recv,
    pair_sems,
    chip_sems,
    line_sems,
    back_line_sems,
    back_chip_sems,
    back_pair_sems,
):
    row, col, rows, cols = place()
    tile = folded.shape[1]
    points = raw.shape[1]
    half = points // 2
    reach = tile + points
    mode_count = probe.shape[0]
    frame_count = raw.shape[0]
    gradient = extended

    loads = [
        pltpu.make_async_copy(source, target, local_sems.at[i])
        for i, (source, target) in enumerate(
            (
                (raw_hbm, raw),
                (delta_hbm, delta),
                (object_hbm, extended.at[:, pl.ds(half, tile), pl.ds(half, tile)]),
                (probe_hbm, probe),
                (forward_hbm, forward),
                (backward_hbm, backward),
            )
        )
    ]
    for load in loads:
        load.start()
    greet()

    lanes_of = lax.broadcasted_iota(jnp.int32, (8, 128), 1)

    def chosen(other):
        pick, top, left, live = (jnp.int32(0), jnp.int32(0), jnp.int32(0), jnp.int32(0))
        for k in range(frame_count):
            hit = tile_row[0, k] == other
            pick = jnp.where(hit, k, pick)
            top = jnp.where(hit, offsets[0, k], top)
            left = jnp.where(hit, offsets[1, k], left)
            live = jnp.where(hit, 1, live)
        return pick, top, left, live

    def info_copy(step, target, other):
        return pltpu.make_async_remote_copy(
            src_ref=info_out.at[step],
            dst_ref=infos.at[target],
            send_sem=info_send.at[step],
            recv_sem=info_recv.at[target],
            device_id=(other, col),
            device_id_type=MESH,
        )

    def slot_copy(step, target, other):
        return pltpu.make_async_remote_copy(
            src_ref=outbox.at[step],
            dst_ref=incoming.at[target],
            send_sem=slot_send.at[step],
            recv_sem=slot_recv.at[target],
            device_id=(other, col),
            device_id_type=MESH,
        )

    def tell(step, carry):
        other = lax.rem(row + step, rows)
        _, top, left, live = chosen(other)
        info = jnp.where(lanes_of == 0, top, jnp.where(lanes_of == 1, left, live))

        @pl.when(step == 0)
        def _():
            infos[row] = info

        @pl.when(step > 0)
        def _():
            info_out[step] = info
            info_copy(step, row, other).start()

        return carry

    lax.fori_loop(0, rows, tell, 0)

    def pick(tall, wide, corner, index, part):
        down, across = DIRECTIONS[index]
        if down and across:
            return corner.at[(down + 1) + (across + 1) // 2, part]
        return wide.at[(down + 1) // 2, part] if down else tall.at[(across + 1) // 2, part]

    def bound_copy(index, part):
        down, across = DIRECTIONS[index]
        return pltpu.make_async_remote_copy(
            src_ref=bound_out.at[part],
            dst_ref=bounds.at[part, index],
            send_sem=bound_send.at[part, index],
            recv_sem=bound_recv.at[part, index],
            device_id=(row + down, col + across),
            device_id_type=MESH,
        )

    def object_halo(index):
        down, across = DIRECTIONS[index]
        if down:
            start, size = {-1: (0, half), 0: (half, tile - points), 1: (tile - half, half)}[across]
            lanes_from, lanes_to = (pl.ds(start, size), pl.ds(half + start, size))
            device = (row + down, col)
        else:
            lanes_from = inner_edge(across, tile, half)
            lanes_to = outer_edge(-across, tile, half)
            device = (row, col + across)
        return pltpu.make_async_remote_copy(
            src_ref=object_hbm.at[:, inner_edge(down, tile, half), lanes_from],
            dst_ref=extended.at[:, outer_edge(-down, tile, half), lanes_to],
            send_sem=object_send.at[index],
            recv_sem=object_recv.at[index],
            device_id=device,
            device_id_type=MESH,
        )

    def strips(down):
        return [DIRECTIONS.index((down, across)) for across in (-1, 1, 0)]

    for down in (-1, 1):

        @pl.when(inside(row + down, col, rows, cols))
        def _():
            for index in strips(down):
                object_halo(index).start()

    for across in (-1, 1):

        @pl.when(inside(row, col + across, rows, cols))
        def _():
            object_halo(DIRECTIONS.index((0, across))).start()

    for index, (down, across) in enumerate(DIRECTIONS):

        @pl.when(jnp.logical_not(inside(row - down, col - across, rows, cols)))
        def _():
            where = (slice(None), outer_edge(-down, tile, half), outer_edge(-across, tile, half))
            extended[where] = jnp.zeros((2, where[1].size, where[2].size), jnp.float32)

    core = lax.rem(row, 2)
    near = 1 - 2 * core
    sides = ((0, -1), (1, 1))

    def pair_relay(side, across):
        source = pl.multiple_of(tile * (1 - core) + half * core, 8)
        target = pl.multiple_of((half + tile) * core, 8)
        lanes_at = outer_edge(across, tile, half)
        return pltpu.make_async_remote_copy(
            src_ref=extended.at[:, pl.ds(source, half), lanes_at],
            dst_ref=extended.at[:, pl.ds(target, half), lanes_at],
            send_sem=relay_sems.at[0, 0, side],
            recv_sem=relay_sems.at[0, 1, side],
            device_id=(row + near, col),
            device_id_type=MESH,
        )

    def line_relay(side, across):
        rows_at = pl.ds(pl.multiple_of((half + tile) * core, 8), half)
        return pltpu.make_async_remote_copy(
            src_ref=extended.at[:, rows_at, pl.ds(tile if across > 0 else half, half)],
            dst_ref=extended.at[:, rows_at, outer_edge(-across, tile, half)],
            send_sem=relay_sems.at[1, 0, side],
            recv_sem=relay_sems.at[1, 1, side],
            device_id=(row, col + across),
            device_id_type=MESH,
        )

    def relayed(act_pair, act_line, sending):
        for side, across in sides:

            @pl.when(inside(row, col + across, rows, cols))
            def _():
                act_pair(pair_relay(side, across))

            toward = across if sending else -across

            @pl.when(inside(row - near, col + toward, rows, cols))
            def _():
                act_line(line_relay(side, across))

    loads[0].wait()
    loads[1].wait()
    identity = (
        lax.broadcasted_iota(jnp.int32, (points, points), 0)
        == lax.broadcasted_iota(jnp.int32, (points, points), 1)
    ).astype(jnp.float32)
    resample = (identity + delta[...]).astype(jnp.bfloat16)

    def measure(step, carry):
        other = lax.rem(row + step, rows)
        pick, _, _, _ = chosen(other)
        first = product(resample, raw[pick]).astype(jnp.bfloat16)
        second = lax.dot_general(
            first, resample, (((1,), (1,)), ((), ())), preferred_element_type=jnp.float32
        )
        amplitude = jnp.sqrt(jnp.maximum(second, 0.0)).astype(jnp.bfloat16)

        @pl.when(step == 0)
        def _():
            incoming[row] = amplitude

        @pl.when(step > 0)
        def _():
            outbox[step] = amplitude
            slot_copy(step, row, other).start()

        return carry

    lax.fori_loop(0, rows, measure, 0)

    def heard(step, carry):
        source = lax.rem(row - step + rows, rows)
        info_copy(step, source, source).wait()
        return carry

    lax.fori_loop(1, rows, heard, 0)
    noted = pltpu.make_async_copy(infos, places, local_sems.at[6])
    noted.start()
    total[...] = jnp.zeros_like(total)
    shifted[...] = jnp.zeros_like(shifted)
    for which in range(2):
        far = 2 * which - 1

        @pl.when((core == which) & inside(row + far, col, rows, cols))
        def _():
            for index in strips(-far)[:2]:
                object_halo(index).wait_recv()

    for side, across in sides:

        @pl.when(inside(row - near, col + across, rows, cols))
        def _():
            line_relay(side, across).start()

    for side, across in sides:

        @pl.when(inside(row, col + across, rows, cols))
        def _():
            object_halo(DIRECTIONS.index((0, -across))).wait_recv()
            pair_relay(side, across).start()

    for which in range(2):
        far = 2 * which - 1

        @pl.when((core == which) & inside(row + far, col, rows, cols))
        def _():
            object_halo(strips(-far)[2]).wait_recv()

        @pl.when(core == which)
        def _():
            for index in strips(far):
                object_halo(index).wait_recv()

    for load in loads[2:]:
        load.wait()
    noted.wait()
    relayed(lambda copy: copy.wait_recv(), lambda copy: copy.wait_recv(), False)

    span_rows, span_cols = (points + 8, points + 128)

    def spot(step):
        source = lax.rem(row - step + rows, rows)
        return source, places[source, 0, 0], places[source, 0, 1], places[source, 0, 2]

    def onward(pair, carry):
        steps = [pair * GROUP + k for k in range(GROUP)]
        spots = [spot(step) for step in steps]
        for step, (_, top, left, _) in zip(steps, spots):
            skip_rows, skip_cols = (lax.rem(top, 8), lax.rem(left, 128))
            across_rows = pl.ds(lax.div(top, 8) * 8, span_rows)
            across_cols = pl.ds(lax.div(left, 128) * 128, span_cols)
            for part in range(2):
                block = extended[part, across_rows, across_cols]
                block = pltpu.roll(block, lax.rem(span_cols - skip_cols, span_cols), 1)
                block = block[:, :points]
                block = pltpu.roll(block, lax.rem(span_rows - skip_rows, span_rows), 0)
                windows[step, part] = block[:points]
        halves = []
        for step in steps:
            for mode in range(mode_count):
                object_real, object_imag = (windows[step, 0], windows[step, 1])
                probe_real, probe_imag = (probe[mode, 0], probe[mode, 1])
                wave = jnp.concatenate(
                    [
                        (probe_real * object_real - probe_imag * object_imag).astype(
                            jnp.bfloat16
                        ),
                        (probe_real * object_imag + probe_imag * object_real).astype(
                            jnp.bfloat16
                        ),
                    ],
                    0,
                )
                halves.append(product(forward[...], wave).astype(jnp.bfloat16))
        intensities = []
        for k in range(GROUP):
            intensity = jnp.zeros((points, points), jnp.float32)
            for mode in range(mode_count):
                half_done = halves[k * mode_count + mode]
                wave_rows = jnp.concatenate([half_done[:points], half_done[points:]], 1)
                field = product(wave_rows, backward[...])
                far_field[k, mode] = field
                squares = field * field
                intensity = intensity + squares[:, :points] + squares[:, points:]
            intensities.append(intensity)
        for step, (source, _, _, _) in zip(steps, spots):

            @pl.when(step > 0)
            def _():
                slot_copy(step, source, source).wait_recv()

        for k, (step, (source, _, _, live)) in enumerate(zip(steps, spots)):
            amplitude = incoming[source].astype(jnp.float32)
            scaling = 1.0 - amplitude / jnp.sqrt(jnp.maximum(intensities[k], 1.0))
            scaling = scaling * live.astype(jnp.float32)
            scaling = jnp.concatenate([scaling, scaling], 1)
            for mode in range(mode_count):
                residuals[step, mode] = (far_field[k, mode] * scaling).astype(jnp.bfloat16)
        return carry

    lax.fori_loop(0, rows // GROUP, onward, 0)

    def back(mode, group, middle, hook):
        def one(index, carry):
            steps = [index * group + k for k in range(group)]
            backs = [
                product(residuals[step, mode], forward[...]).astype(jnp.bfloat16)
                for step in steps
            ]
            updates = [
                product(
                    backward[...], jnp.concatenate([rows_[:, :points], rows_[:, points:]], 0)
                )
                for rows_ in backs
            ]
            sum_real = total[mode, :points]
            sum_imag = total[mode, points:]
            for step, update in zip(steps, updates):
                update_real, update_imag = (update[:points], update[points:])
                object_real, object_imag = (windows[step, 0], windows[step, 1])
                probe_real, probe_imag = (probe[mode, 0], probe[mode, 1])
                term_real = probe_real * update_real + probe_imag * update_imag
                term_imag = probe_real * update_imag - probe_imag * update_real
                if mode == 0:
                    terms[step, 0] = term_real
                    terms[step, 1] = term_imag
                else:
                    terms[step, 0] += term_real
                    terms[step, 1] += term_imag
                sum_real = sum_real + (object_real * update_real + object_imag * update_imag)
                sum_imag = sum_imag + (object_real * update_imag - object_imag * update_real)
            total[mode, :points] = sum_real
            total[mode, points:] = sum_imag
            if hook:

                @pl.when(index == middle)
                def _():
                    for piece in hook:
                        advance(piece)

            return carry

        return one

    ways = shifted.shape[0]

    def accumulate(part, group):
        chunk = 32
        first = group * ways
        found = [spot(first + k) for k in range(ways)]
        bases = [tile // 8 - lax.div(top, 8) for _, top, _, _ in found]
        acrosses = [(tile // 128 - 1 - lax.div(left, 128)) * 128 for _, _, left, _ in found]
        for k in range(ways):
            _, top, left, _ = found[k]
            block = jnp.concatenate(
                [terms[first + k, part], jnp.zeros((8, points), jnp.float32)], 0
            )
            block = pltpu.roll(block, lax.rem(top, 8), 0)
            block = jnp.concatenate([block, jnp.zeros((span_rows, 128), jnp.float32)], 1)
            shifted[k, pl.ds(tile, span_rows), pl.ds(tile - 128, span_cols)] = pltpu.roll(
                block, lax.rem(left, 128), 1
            )

        def add(index, inner):
            start = pl.multiple_of(index * chunk, 8)
            value = gradient[part, pl.ds(start, chunk)]
            for k in range(ways):
                source = (bases[k] + index * (chunk // 8)) * 8
                value = value + shifted[k, pl.ds(source, chunk), pl.ds(acrosses[k], reach)]
            gradient[part, pl.ds(start, chunk)] = value
            return inner

        lax.fori_loop(0, reach // chunk, add, 0)

    pieces = pair_in.shape[0]
    length = pair_in.shape[1]
    chips = rows // 2
    chip = row // 2
    norming = 1.0 / math.sqrt(frame_count * rows * cols)

    def folded_copy(part):
        return pltpu.make_async_copy(folded.at[part], folded_out.at[part], out_sems.at[0, part])

    def summed_copy(piece):
        return pltpu.make_async_copy(
            summed.at[piece], summed_out.at[piece], out_sems.at[1, piece]
        )

    chip_rows = length // chips
    line_rows = chip_rows // cols
    lanes = summed.shape[2] // 2

    def own_half():
        return pl.ds(pl.multiple_of(core * lanes, lanes), lanes)

    def sibling_half():
        return pl.ds(pl.multiple_of((1 - core) * lanes, lanes), lanes)

    sibling = (row + 1 - 2 * core, col)
    def halo(index, part):
        down, across = DIRECTIONS[index]
        return pltpu.make_async_remote_copy(
            src_ref=pick(code_tall, code_wide, code_corners, index, part),
            dst_ref=pick(halos_tall, halos_wide, corners, index, part),
            send_sem=halo_send.at[part, index],
            recv_sem=halo_recv.at[part, index],
            device_id=(row + down, col + across),
            device_id_type=MESH,
        )

    def encode(part, bound):
        for index, (down, across) in enumerate(DIRECTIONS):
            where = (part, outer_edge(down, tile, half), outer_edge(across, tile, half))
            pick(code_tall, code_wide, code_corners, index, part)[...] = coded(
                gradient[where], bound
            )

    def start_halos(part, wanted=(-1, 0, 1)):
        for index, (down, across) in enumerate(DIRECTIONS):
            if down not in wanted:
                continue

            @pl.when(inside(row + down, col + across, rows, cols))
            def _():
                bound_copy(index, part).start()
                halo(index, part).start()

    def take_halos(part):
        for index, (down, across) in enumerate(DIRECTIONS):

            @pl.when(inside(row - down, col - across, rows, cols))
            def _():
                bound_copy(index, part).wait_recv()
                halo(index, part).wait_recv()
                where = (part, inner_edge(-down, tile, half), inner_edge(-across, tile, half))
                folded[where] += decoded(
                    pick(halos_tall, halos_wide, corners, index, part)[...],
                    jnp.max(bounds[part, index]),
                )

    def remote(source, target, sems, index, device):
        return pltpu.make_async_remote_copy(
            src_ref=source,
            dst_ref=target,
            send_sem=sems.at[0, index],
            recv_sem=sems.at[1, index],
            device_id=device,
            device_id_type=MESH,
        )

    def pair_copy(piece):
        return remote(
            total.at[piece, :, sibling_half()], pair_in.at[piece], pair_sems, piece, sibling
        )

    def chip_copy(piece, step):
        other = lax.rem(chip + step, chips)
        start = pl.multiple_of(other * chip_rows, 8)
        index = piece * chips + step
        return remote(
            pair_sum.at[piece, pl.ds(start, chip_rows)],
            chip_in.at[index],
            chip_sems,
            index,
            (2 * other + core, col),
        )

    def line_copy(piece, step):
        other = lax.rem(col + step, cols)
        start = pl.multiple_of(other * line_rows, 8)
        index = piece * cols + step
        return remote(
            chip_sum.at[piece, pl.ds(start, line_rows)],
            line_in.at[index],
            line_sems,
            index,
            (row, other),
        )

    def back_line_copy(piece, step):
        other = lax.rem(col + step, cols)
        start = pl.multiple_of(col * line_rows, 8)
        return remote(
            line_sum.at[piece],
            line_out.at[piece, pl.ds(start, line_rows)],
            back_line_sems,
            piece * cols + step,
            (row, other),
        )

    def back_chip_copy(piece, step):
        other = lax.rem(chip + step, chips)
        start = pl.multiple_of(chip * chip_rows, 8)
        return remote(
            line_out.at[piece],
            chip_out.at[piece, pl.ds(start, chip_rows)],
            back_chip_sems,
            piece * chips + step,
            (2 * other + core, col),
        )

    def back_pair_copy(piece):
        return remote(
            chip_out.at[piece],
            summed.at[piece, :, own_half()],
            back_pair_sems,
            piece,
            sibling,
        )

    def pair_stage(piece):
        pair_copy(piece).wait_recv()
        pair_sum[piece] = total[piece, :, own_half()] + pair_in[piece]
        for step in range(1, chips):
            chip_copy(piece, step).start()

    def chip_stage(piece):
        start = pl.multiple_of(chip * chip_rows, 8)
        value = pair_sum[piece, pl.ds(start, chip_rows)]
        for step in range(1, chips):
            chip_copy(piece, step).wait_recv()
            value = value + chip_in[piece * chips + step]
        chip_sum[piece] = value
        for step in range(1, cols):
            line_copy(piece, step).start()

    def line_stage(piece):
        start = pl.multiple_of(col * line_rows, 8)
        value = chip_sum[piece, pl.ds(start, line_rows)]
        for step in range(1, cols):
            line_copy(piece, step).wait_recv()
            value = value + line_in[piece * cols + step]
        value = value * norming
        line_sum[piece] = value
        line_out[piece, pl.ds(start, line_rows)] = value
        for step in range(1, cols):
            back_line_copy(piece, step).start()

    def back_line_stage(piece):
        for step in range(1, cols):
            back_line_copy(piece, step).wait_recv()
        start = pl.multiple_of(chip * chip_rows, 8)
        for step in range(1, chips):
            back_chip_copy(piece, step).start()
        chip_out[piece, pl.ds(start, chip_rows)] = line_out[piece]

    def back_chip_stage(piece):
        for step in range(1, chips):
            back_chip_copy(piece, step).wait_recv()
        back_pair_copy(piece).start()
        summed[piece, :, own_half()] = chip_out[piece]

    stages = (pair_stage, chip_stage, line_stage, back_line_stage, back_chip_stage)
    reached = [0] * pieces

    def advance(piece):
        if reached[piece] < len(stages):
            stages[reached[piece]](piece)
            reached[piece] += 1

    middle = rows // 2 // BACK_GROUP - 1
    for mode in range(mode_count):
        hook = (mode - 1,) if mode else ()
        lax.fori_loop(0, rows // BACK_GROUP, back(mode, BACK_GROUP, middle, hook), 0)
        pair_copy(mode).start()
    advance(0)

    for index, (down, across) in enumerate(DIRECTIONS):

        @pl.when(inside(row + down, col + (0 if down else across), rows, cols))
        def _():
            object_halo(index).wait_send()

    relayed(lambda copy: copy.wait_send(), lambda copy: copy.wait_send(), True)

    gradient[...] = jnp.zeros_like(gradient)
    passes = rows // ways
    for part, which in enumerate(((0, 1, 2), (0, 1, 2))):
        for group in range(passes):
            accumulate(part, group)
            if group == (passes - 1) // 2:
                for piece in which:
                    advance(piece)
        bound = greatest(gradient[part])
        bound_out[part] = jnp.full((8, 128), bound, jnp.float32)
        encode(part, bound)
        if part == 0:
            start_halos(0)
    advance(1)
    advance(2)
    start_halos(1, (0,))
    advance(0)
    folded[...] = gradient[:, half : half + tile, half : half + tile]
    advance(2)
    start_halos(1, (-1, 1))
    take_halos(0)
    folded_copy(0).start()
    for _ in stages:
        for piece in range(pieces):
            advance(piece)
    take_halos(1)
    folded_copy(1).start()
    for piece in range(pieces):
        back_pair_copy(piece).wait_recv()
        summed_copy(piece).start()
    for index, (down, across) in enumerate(DIRECTIONS):

        @pl.when(inside(row + down, col + across, rows, cols))
        def _():
            bound_copy(index, 0).wait_send()
            bound_copy(index, 1).wait_send()
            halo(index, 0).wait_send()
            halo(index, 1).wait_send()

    def sent(step, carry):
        slot_copy(step, row, lax.rem(row + step, rows)).wait_send()
        return carry

    lax.fori_loop(1, rows, sent, 0)
    for piece in range(pieces):
        pair_copy(piece).wait_send()
        back_pair_copy(piece).wait_send()
        for step in range(1, chips):
            chip_copy(piece, step).wait_send()
            back_chip_copy(piece, step).wait_send()
        for step in range(1, cols):
            line_copy(piece, step).wait_send()
            back_line_copy(piece, step).wait_send()
    for part in range(2):
        folded_copy(part).wait()
    for piece in range(pieces):
        summed_copy(piece).wait()


def whole(tile_row, offsets, object_field, probe, raw_counts, delta, forward, backward):
    rows, cols = (lax.axis_size("row"), lax.axis_size("col"))
    tile = object_field.shape[1]
    modes, _, points, _ = probe.shape
    half = points // 2
    reach = tile + points
    length, lanes = (2 * points, points // 2)
    chips = rows // 2
    f32, bf16, i32, i16 = (jnp.float32, jnp.bfloat16, jnp.int32, jnp.int16)
    vmem = pl.BlockSpec(memory_space=pltpu.VMEM)
    hbm = pl.BlockSpec(memory_space=pl.ANY)
    dma = pltpu.SemaphoreType.DMA
    return pl.pallas_call(
        whole_kernel,
        name="whole",
        out_shape=(
            jax.ShapeDtypeStruct((2, tile, tile), f32),
            jax.ShapeDtypeStruct((modes, length, points), f32),
        ),
        in_specs=[pl.BlockSpec(memory_space=pltpu.SMEM)] * 2 + [hbm] * 6,
        out_specs=(hbm, hbm),
        scratch_shapes=[
            pltpu.VMEM((2, tile, tile), f32),
            pltpu.VMEM((modes, length, points), f32),
            dma((2, max(2, modes))),
            pltpu.VMEM(probe.shape, f32),
            pltpu.VMEM(raw_counts.shape, bf16),
            pltpu.VMEM(delta.shape, f32),
            pltpu.VMEM(forward.shape, bf16),
            pltpu.VMEM(backward.shape, bf16),
            pltpu.VMEM((2, reach, reach), f32),
            pltpu.VMEM((rows, points, points), bf16),
            pltpu.VMEM((rows, points, points), bf16),
            pltpu.VMEM((rows, 8, 128), i32),
            pltpu.VMEM((rows, 8, 128), i32),
            pltpu.SMEM((rows, 8, 128), i32),
            pltpu.VMEM((rows, 2, points, points), f32),
            pltpu.VMEM((rows, modes, points, 2 * points), bf16),
            pltpu.VMEM((GROUP, modes, points, 2 * points), f32),
            pltpu.VMEM((rows, 2, points, points), f32),
            pltpu.VMEM((modes, length, points), f32),
            pltpu.VMEM((WAYS if rows <= 8 else 1, 2 * tile + points, 2 * tile + half), f32),
            pltpu.VMEM((2, 2, tile, half), i16),
            pltpu.VMEM((2, 2, half, tile), i16),
            pltpu.VMEM((4, 2, half, half), i16),
            pltpu.VMEM((2, 2, tile, half), i16),
            pltpu.VMEM((2, 2, half, tile), i16),
            pltpu.VMEM((4, 2, half, half), i16),
            pltpu.VMEM((2, 8, 128), f32),
            pltpu.VMEM((2, 8, 8, 128), f32),
            pltpu.VMEM((modes, length, lanes), f32),
            pltpu.VMEM((modes, length, lanes), f32),
            pltpu.VMEM((modes * chips, length // chips, lanes), f32),
            pltpu.VMEM((modes, length // chips, lanes), f32),
            pltpu.VMEM((modes * cols, length // chips // cols, lanes), f32),
            pltpu.VMEM((modes, length // chips // cols, lanes), f32),
            pltpu.VMEM((modes, length // chips, lanes), f32),
            pltpu.VMEM((modes, length, lanes), f32),
            dma((7,)),
            dma((8,)),
            dma((8,)),
            dma((2, 2, 2)),
            dma((rows,)),
            dma((rows,)),
            dma((rows,)),
            dma((rows,)),
            dma((2, 8)),
            dma((2, 8)),
            dma((2, 8)),
            dma((2, 8)),
            dma((2, modes)),
            dma((2, modes * chips)),
            dma((2, modes * cols)),
            dma((2, modes * cols)),
            dma((2, modes * chips)),
            dma((2, modes)),
        ],
        compiler_params=pltpu.CompilerParams(
            collective_id=0, has_side_effects=True, vmem_limit_bytes=67043328
        ),
    )(tile_row, offsets, object_field, probe, raw_counts, delta, forward, backward)


def finish_kernel(folded_in, summed_in, folded_out, summed_out, folded, summed, sems):
    moves = [(folded_in, folded, folded_out, part) for part in range(folded.shape[0])]
    moves += [(summed_in, summed, summed_out, piece) for piece in range(summed.shape[0])]
    loads = []
    stores = []
    for i, (source, held, target, k) in enumerate(moves):
        loads.append(pltpu.make_async_copy(source.at[k], held.at[k], sems.at[0, i]))
        stores.append(pltpu.make_async_copy(held.at[k], target.at[k], sems.at[1, i]))
    for load in loads:
        load.start()
    for load, store in zip(loads, stores):
        load.wait()
        store.start()
    for store in stores:
        store.wait()


def finish(folded, summed):
    hbm = pl.BlockSpec(memory_space=pl.ANY)
    return pl.pallas_call(
        finish_kernel,
        name="finish",
        out_shape=(
            jax.ShapeDtypeStruct(folded.shape, folded.dtype),
            jax.ShapeDtypeStruct(summed.shape, summed.dtype),
        ),
        in_specs=[hbm, hbm],
        out_specs=(hbm, hbm),
        scratch_shapes=[
            pltpu.VMEM(folded.shape, folded.dtype),
            pltpu.VMEM(summed.shape, summed.dtype),
            pltpu.SemaphoreType.DMA((2, folded.shape[0] + summed.shape[0])),
        ],
    )(folded, summed)


def shards(object_field, probe, raw_counts, resample_delta, tile_row, offsets):
    points = probe.shape[-1]
    forward, backward = dft_tables(points)
    object_grad, summed = whole(
        tile_row.T, offsets.T, object_field, probe, raw_counts, resample_delta, forward, backward
    )
    object_grad, summed = finish(object_grad, summed)
    return (object_grad, summed.reshape(probe.shape))


def solution(mesh):
    placed = (
        P(None, "row", "col"),
        P(),
        P(("row", "col"), None, None),
        P(),
        P(("row", "col"), None),
        P(("row", "col"), None),
    )
    return jax.shard_map(
        shards, mesh=mesh, in_specs=placed, out_specs=(P(None, "row", "col"), P()), check_vma=False
    )
```
